256 devices in a mesh: cosmo: 2 (over z), row: 128 (over y, x, core).
Axes of the slice: x: 8, y: 8, z: 2, core: 2. Of those that a mesh axis runs over, the one named last changes fastest.
The devices are a block of a 8x8x16 slice.
Arguments:
- potentials: float32 [4, 2048, 16384], P('cosmo', 'row'), parts along dimension 0, may hold values from -3 to 3
- ratios: float32 [6], P('cosmo'), parts along dimension 0, may hold values from 0.3 to 0.9
- row_offset: int32 [256], P('cosmo'), parts along dimension 0, may hold values from 0 to 7
- col_offset: int32 [256], P('cosmo'), parts along dimension 0, may hold values from 0 to 127
Outputs:
- convergence: float32 [4096, 16384], P(('cosmo', 'row')), parts along dimension 0
- shear_map: float32 [2, 4096, 16384], P(None, ('cosmo', 'row')), parts along dimension 1
- rotation: float32 [4096, 16384], P(('cosmo', 'row')), parts along dimension 0
- displacement: float32 [2, 4096, 16384], P(None, ('cosmo', 'row')), parts along dimension 1
The draws below stay inside these ranges and needn't reach their ends.
There are 2 independent parts, one for each index of `cosmo`. The reference program is written for one: setup_inputs(seed, part) draws one part's arguments, and reference() takes and returns one part's arrays. A program takes and returns all parts, laid end to end along the dimension named above; each array names one. Nothing has to cross between parts.
Inputs may be any that keep to these rules, and one draw needn't show every extreme that they name: `row_offset`: row offsets count blocks of 256 rows.
All inputs are finite; a program needn't handle non-finite values.
Results may differ from the reference program's by a relative error of at most 0.00002.
Values sent between devices are 32-bit elements; how exact they have to be, the bound alone decides.
A program may use at most 128 MiB of HBM per device.

```python
import jax
import jax.numpy as jnp

NC = 16384
PLANES = 2
RB = 8
NR = 2048
NCB = 128


def plant(entries, own_key, smallest, high):
    spot = [jax.random.randint(jax.random.fold_in(own_key, axis), (), 0, length) for axis, length in enumerate(entries.shape)]
    main_axis = entries.shape.index(max(entries.shape))
    neighbour = spot[:main_axis] + [(spot[main_axis] + 1) % entries.shape[main_axis]] + spot[main_axis + 1:]
    return entries.at[tuple(spot)].set(smallest).at[tuple(neighbour)].set(high)


def level_of(key, dims, split, smallest, largest):
    level = 1.0
    for position, shards_of in split:
        draws = jax.random.uniform(jax.random.fold_in(jax.random.fold_in(key, 6), position), (shards_of,), jnp.float32, smallest / len(split), largest / len(split))
        level = level * jnp.repeat(jnp.exp(draws), dims[position] // shards_of).reshape((-1,) + (1,) * (len(dims) - 1 - position))
    return level


def centred(own_key, shape, spread, reach, cuts=(), kind=jnp.bfloat16):
    values = jax.random.normal(own_key, shape, jnp.float32) * spread
    if len(cuts) > 0:
        values = level_of(own_key, shape, cuts, -0.22, 0.18) * values
    return jnp.clip(values, min=-reach, max=reach).astype(kind)


def setup_inputs(seed: int = 0, part: int = 0) -> dict:
    splits = jax.random.split(jax.random.key(seed), 5)
    part_keys = jax.random.split(jax.random.fold_in(splits[4], part), 5)
    potentials = centred(part_keys[0], (PLANES, NR, NC), 0.5, 3.0, ((1, 128),), jnp.float32)
    ratios = jnp.clip(jax.random.uniform(part_keys[1], (3,), jnp.float32, 0.3, 0.9), 0.3, 0.9)
    row_offset = plant(jax.random.randint(part_keys[2], (NCB,), 0, RB), jax.random.fold_in(part_keys[2], 1), 0, RB - 1).astype(jnp.int32)
    col_offset = plant(jax.random.randint(part_keys[3], (NCB,), 0, NCB), jax.random.fold_in(part_keys[3], 1), 0, NCB - 1).astype(jnp.int32)
    return {"potentials": potentials, "ratios": ratios, "row_offset": row_offset, "col_offset": col_offset}


def slope_along(field, direction):
    return (8.0 * (jnp.roll(field, -1, direction) - jnp.roll(field, 1, direction)) - (jnp.roll(field, -2, direction) - jnp.roll(field, 2, direction))) / 12.0


def derive_plane(potential):
    slope_r = slope_along(potential, 0)
    slope_c = slope_along(potential, 1)
    return (slope_r, slope_c, slope_along(slope_r, 0), slope_along(slope_r, 1), slope_along(slope_c, 1))


def assemble(nearer, farther, ratios):
    near_r, near_c, near_rr, near_rc, near_cc = nearer
    far_r, far_c, far_rr, far_rc, far_cc = farther
    beta_near = ratios[0]
    beta_one = ratios[1]
    beta_two = ratios[2]
    inner_rr = 1.0 - beta_near * near_rr
    inner_rc = -beta_near * near_rc
    inner_cc = 1.0 - beta_near * near_cc
    chain_rr = far_rr * inner_rr + far_rc * inner_rc
    chain_rc = far_rr * inner_rc + far_rc * inner_cc
    chain_cr = far_rc * inner_rr + far_cc * inner_rc
    chain_cc = far_rc * inner_rc + far_cc * inner_cc
    total_rr = 1.0 - beta_one * near_rr - beta_two * chain_rr
    total_rc = -beta_one * near_rc - beta_two * chain_rc
    total_cr = -beta_one * near_rc - beta_two * chain_cr
    total_cc = 1.0 - beta_one * near_cc - beta_two * chain_cc
    convergence = 1.0 - 0.5 * (total_rr + total_cc)
    shear_map = jnp.stack([0.5 * (total_rr - total_cc), -0.5 * (total_rc + total_cr)])
    rotation = 0.5 * (total_rc - total_cr)
    displacement = jnp.stack([beta_one * near_r + beta_two * far_r, beta_one * near_c + beta_two * far_c])
    return convergence, shear_map, rotation, displacement


def reference(potentials, ratios, row_offset, col_offset):
    nearer = derive_plane(potentials[0])
    derived = derive_plane(potentials[1])
    blocks = NC // 128
    source = (jnp.arange(blocks, dtype=jnp.int32) + col_offset.astype(jnp.int32)) % blocks
    lookup_rows = (jnp.arange(NR, dtype=jnp.int32)[:, None] + (NR // RB) * row_offset.astype(jnp.int32)[None, :]) % NR

    def sample(field):
        strips = field.reshape(NR, blocks, 128)
        return strips[lookup_rows, source[None, :], :].reshape(NR, NC)

    farther = tuple(sample(member) for member in derived)
    return assemble(nearer, farther, ratios)
```

```python
import functools

import jax
import jax.numpy as jnp
from jax import lax
from jax.experimental import pallas as pl
from jax.experimental.pallas import tpu as pltpu
from jax.sharding import PartitionSpec as P

RB = 8
LANES = 128
HALF = RB // 2
GROUP = 16
MESH = pl.DeviceIdType.MESH

PLANS = ((4, 3, 2, 1), (8, 8, 8, 4))


def chunk_base(plan):
    base, total = [], 0
    for count in plan:
        base.append(total)
        total += count
    return base, total


def iota(shape, dim):
    return lax.broadcasted_iota(jnp.int32, shape, dim)


def table_kernel(row_ref, col_ref, tab_ref):
    blocks = row_ref.shape[1]
    f32 = jnp.float32
    row = row_ref[...].astype(f32)
    lane = iota((1, blocks), 1)
    lane_f = lane.astype(f32)
    source = lane_f + col_ref[...].astype(f32)
    source = jnp.where(source >= blocks, source - blocks, source)
    sub2 = iota((blocks, blocks), 0)
    lane2 = iota((blocks, blocks), 1)

    def column(v):
        return jnp.sum(jnp.where(sub2 == lane2, jnp.broadcast_to(v, (blocks, blocks)), 0.0), axis=1, keepdims=True)

    def total(v):
        return jnp.sum(v, axis=1, keepdims=True)

    halfway = (row == HALF).astype(f32)
    dist = jnp.where(row <= HALF, row, RB - row)
    n_half = total(halfway)
    load_a = total(jnp.where(row < HALF, row, 0.0))
    load_b = total(jnp.where(row > HALF, RB - row, 0.0))
    take_a = jnp.clip(jnp.floor((load_b + HALF * n_half - load_a) / (2 * HALF) + 0.5), 0.0, n_half)
    rank_half = jnp.sum(jnp.where(sub2 < lane2, jnp.broadcast_to(column(halfway), (blocks, blocks)), 0.0), axis=0, keepdims=True)
    way = jnp.where(row == 0, 0.0, jnp.where(row < HALF, 1.0, 2.0))
    way = jnp.where((row == HALF) & (rank_half < take_a), 1.0, way)
    big = 4096.0
    key = way * big + (HALF - dist) * blocks + lane_f
    key_c = jnp.broadcast_to(column(key), (blocks, blocks))
    key_r = jnp.broadcast_to(key, (blocks, blocks))
    way_r = jnp.broadcast_to(way, (blocks, blocks))
    ahead = (key_c < key_r) & (key_c >= way_r * big)
    slot = jnp.sum(ahead.astype(f32), axis=0, keepdims=True)
    slot_c = jnp.broadcast_to(column(slot), (blocks, blocks))
    way_c = jnp.broadcast_to(column(way), (blocks, blocks))
    source_c = jnp.broadcast_to(column(source), (blocks, blocks))
    here = slot_c == lane2.astype(f32)
    send = [
        jnp.sum(jnp.where(here & (way_c == w), source_c, 0.0), axis=0, keepdims=True) for w in (1.0, 2.0)
    ]
    fits = jnp.ones((1, 1), f32)
    for hop, count in enumerate(PLANS[0]):
        for w in (1.0, 2.0):
            need = total(((way == w) & (dist > hop)).astype(f32))
            fits = jnp.where(need > count * GROUP, 0.0, fits)
    chunk = jnp.floor(slot / GROUP)
    within = slot - chunk * GROUP
    spot = []
    for plan in PLANS:
        base, number = chunk_base(plan)
        at = jnp.zeros((1, blocks), f32)
        for hop in range(HALF):
            at = jnp.where(dist == hop + 1, float(base[hop]), at)
        spot.append(at + chunk + jnp.where(way == 2.0, float(number), 0.0))
    spot = jnp.where(fits > 0, spot[0], spot[1])
    spot = jnp.where(way == 0, 0.0, spot)
    within = jnp.where(way == 0, 0.0, within)
    turn = 8.0 * (lane_f - GROUP * jnp.floor(lane_f / GROUP) - within)
    turn = jnp.where(turn < 0, turn + LANES, turn)
    rows = [
        send[0],
        send[1],
        spot * (GROUP + 1) + within,
        spot * (GROUP + 1) + GROUP,
        turn,
        source,
        (way == 0).astype(f32),
        jnp.broadcast_to(1.0 - fits, (1, blocks)),
    ]
    tab_ref[...] = jnp.concatenate(rows, axis=0).astype(jnp.int32)


def exchange_kernel(plan, tab, pot, w_ref, h_ref, h1_ref, p1, p2, tiles, sent, got, en, ep, gn, gp, en1, ep1, gn1, gp1,
                    local_sem, send_sem, recv_sem, edge_send, edge_recv):
    base, number = chunk_base(plan)
    size = lax.axis_size("row")
    stride = size // RB
    me = lax.axis_index("row")
    blocks = p2.shape[1] // LANES
    rows = p2.shape[0]
    top = rows - 8
    packet = GROUP + 1
    first = plan[0]

    load2 = pltpu.make_async_copy(pot.at[1], p2, local_sem.at[0])
    load1 = pltpu.make_async_copy(pot.at[0], p1, local_sem.at[1])
    load2.start()
    load1.start()
    barrier = pltpu.get_barrier_semaphore()
    for by in (stride, size - stride, 1, size - 1):
        pl.semaphore_signal(barrier, inc=1, device_id={"row": lax.rem(me + by, size)}, device_id_type=MESH)

    lane = iota((rows, LANES), 1)
    lane_group = lane // 8
    sub = iota((8, LANES), 0)

    def tile(ref, s):
        return ref[s]

    def split(i, carry):
        for j in range(GROUP):
            tiles[i * GROUP + j] = p2[:, pl.ds(pl.multiple_of((i * GROUP + j) * LANES, LANES), LANES)]
        return carry

    def sides(ref, s):
        before = tile(ref, lax.rem(s + (blocks - 1), blocks))
        after = tile(ref, lax.rem(s + 1, blocks))
        return jnp.where(lane >= LANES // 2, before, after)

    def pack(i):
        way = lax.rem(i, 2)
        chunk = i // 2
        halo = jnp.zeros((rows, LANES), jnp.float32)
        for j in range(GROUP):
            s = tab[way, chunk * GROUP + j]
            sent[i * packet + j] = tile(tiles, s)
            halo = jnp.where(lane_group == j, pltpu.roll(sides(tiles, s), (8 * j + 4) % LANES, 1), halo)
        sent[i * packet + GROUP] = halo

    def toward(way):
        return {"row": lax.rem(me + jnp.where(way == 0, size - stride, stride), size)}

    def first_copy(i):
        way = lax.rem(i, 2)
        to = way * number + i // 2
        return pltpu.make_async_remote_copy(
            src_ref=sent.at[pl.ds(i * packet, packet)],
            dst_ref=got.at[pl.ds(to * packet, packet)],
            send_sem=send_sem.at[to],
            recv_sem=recv_sem.at[to],
            device_id=toward(way),
            device_id_type=MESH,
        )

    def relay(way, hop, c):
        origin = way * number + base[hop - 1] + c
        to = way * number + base[hop] + c
        return pltpu.make_async_remote_copy(
            src_ref=got.at[pl.ds(origin * packet, packet)],
            dst_ref=got.at[pl.ds(to * packet, packet)],
            send_sem=send_sem.at[to],
            recv_sem=recv_sem.at[to],
            device_id={"row": lax.rem(me + (size - stride if way == 0 else stride), size)},
            device_id_type=MESH,
        )

    def arrival(to):
        piece = got.at[pl.ds(to * packet, packet)]
        return pltpu.make_async_remote_copy(
            src_ref=piece, dst_ref=piece, send_sem=send_sem.at[to], recv_sem=recv_sem.at[to],
            device_id={"row": lax.rem(me + stride, size)}, device_id_type=MESH,
        )

    def edge(src, dst, by, at):
        return pltpu.make_async_remote_copy(
            src_ref=src, dst_ref=dst, send_sem=edge_send.at[at], recv_sem=edge_recv.at[at],
            device_id={"row": lax.rem(me + by, size)}, device_id_type=MESH,
        )

    load2.wait()
    lax.fori_loop(0, blocks // GROUP, split, 0)
    pack(0)
    pl.semaphore_wait(barrier, 4)

    def step(i, carry):
        pack(i)
        first_copy(i - 1).start()
        return carry

    lax.fori_loop(1, 2 * first, step, 0)
    first_copy(2 * first - 1).start()

    load1.wait()
    half = p1.shape[1] // 2
    width = 1024
    sub_w = iota((8, width), 0)

    def edges1(i, carry):
        at = pl.multiple_of(i * width, width)
        here, there = pl.ds(at, width), pl.ds(pl.multiple_of(at + half, width), width)
        en1[:, here] = jnp.where(sub_w >= 4, p1[top:, here], pltpu.roll(p1[top:, there], 4, 0))
        ep1[:, here] = jnp.where(sub_w < 4, p1[:8, here], pltpu.roll(p1[:8, there], 4, 0))
        return carry

    lax.fori_loop(0, half // width, edges1, 0)
    edge_down1 = edge(en1, gn1, 1, 0)
    edge_up1 = edge(ep1, gp1, size - 1, 1)

    for hop in range(1, HALF):
        for c in range(plan[hop]):
            for way in range(2):
                arrival(way * number + base[hop - 1] + c).wait_recv()
                relay(way, hop, c).start()
        if hop == 1:
            edge_down1.start()
            edge_up1.start()

    edge_down1.wait_recv()
    edge_up1.wait_recv()

    def halo1(i, carry):
        at = pl.multiple_of(i * width, width)
        here, there = pl.ds(at, width), pl.ds(pl.multiple_of(at + half, width), width)
        down, up = gn1[:, here], gp1[:, here]
        h1_ref[:, here] = jnp.where(sub_w >= 4, down, up)
        h1_ref[:, there] = pltpu.roll(jnp.where(sub_w < 4, down, up), 4, 0)
        return carry

    lax.fori_loop(0, half // width, halo1, 0)

    for hop in range(HALF):
        for c in range(plan[hop + 1] if hop + 1 < HALF else 0, plan[hop]):
            for way in range(2):
                arrival(way * number + base[hop] + c).wait_recv()

    quarter = blocks // GROUP // 2

    def fetch(b, j, halo):
        own = jnp.full((rows, LANES), tab[6, b], jnp.int32) > 0
        s = tab[5, b]
        value = jnp.where(own, tile(tiles, s), got[tab[2, b]])
        mine = pltpu.roll(sides(tiles, s), (8 * j + 4) % LANES, 1)
        theirs = got[tab[3, b]]
        turn = jnp.full((rows, LANES), tab[4, b], jnp.int32)
        for bit in (8, 16, 32, 64):
            theirs = jnp.where((turn & bit) != 0, pltpu.roll(theirs, bit, 1), theirs)
        halo = jnp.where(lane_group == j, jnp.where(own, mine, theirs), halo)
        return value, halo

    def settle(g, carry):
        halo_a = jnp.zeros((rows, LANES), jnp.float32)
        halo_b = jnp.zeros((rows, LANES), jnp.float32)
        for j in range(GROUP + 1):
            if j < GROUP:
                a, halo_a = fetch(g * GROUP + j, j, halo_a)
                b, halo_b = fetch((g + quarter) * GROUP + j, j, halo_b)
            else:
                a, b = halo_a, halo_b
            w_ref[g * packet + j] = a
            w_ref[(g + quarter) * packet + j] = b
            en[g * packet + j] = jnp.where(sub >= 4, a[top:], pltpu.roll(b[top:], 4, 0))
            ep[g * packet + j] = jnp.where(sub < 4, a[:8], pltpu.roll(b[:8], 4, 0))
        return carry

    lax.fori_loop(0, quarter, settle, 0)
    part = [pl.ds(g * packet, packet) for g in range(quarter)]
    edges = [
        (edge(en.at[part[g]], gn.at[part[g]], 1, 2 + 2 * g), edge(ep.at[part[g]], gp.at[part[g]], size - 1, 3 + 2 * g))
        for g in range(quarter)
    ]
    for down, up in edges:
        down.start()
        up.start()
    for g in range(quarter):
        edges[g][0].wait_recv()
        edges[g][1].wait_recv()
        for j in range(packet):
            down, up = gn[g * packet + j], gp[g * packet + j]
            h_ref[g * packet + j] = jnp.where(sub >= 4, down, up)
            h_ref[(g + quarter) * packet + j] = pltpu.roll(jnp.where(sub < 4, down, up), 4, 0)

    edge_down1.wait_send()
    edge_up1.wait_send()
    for down, up in edges:
        down.wait_send()
        up.wait_send()
    for to in range(2 * number):
        arrival(to).wait_send()


def exchange(index, tab, potentials):
    plan = PLANS[index]
    rows, columns = potentials.shape[1:]
    blocks = columns // LANES
    _, number = chunk_base(plan)
    groups = blocks // GROUP
    packet = GROUP + 1
    f32 = jnp.float32
    pairs = groups // 2 * packet
    edge = pltpu.VMEM((pairs, 8, LANES), f32)
    edge1 = pltpu.VMEM((8, columns // 2), f32)
    vmem = pl.BlockSpec(memory_space=pltpu.VMEM)
    return pl.pallas_call(
        functools.partial(exchange_kernel, plan),
        out_shape=(
            jax.ShapeDtypeStruct((groups * packet, rows, LANES), f32),
            jax.ShapeDtypeStruct((groups * packet, 8, LANES), f32),
            jax.ShapeDtypeStruct((8, columns), f32),
        ),
        in_specs=[pl.BlockSpec(memory_space=pltpu.SMEM), pl.BlockSpec(memory_space=pl.ANY)],
        out_specs=(vmem, vmem, vmem),
        scratch_shapes=[
            pltpu.VMEM((rows, columns), f32),
            pltpu.VMEM((rows, columns), f32),
            pltpu.VMEM((blocks, rows, LANES), f32),
            pltpu.VMEM((2 * plan[0] * packet, rows, LANES), f32),
            pltpu.VMEM((2 * number * packet, rows, LANES), f32),
            edge, edge, edge, edge,
            edge1, edge1, edge1, edge1,
            pltpu.SemaphoreType.DMA((2,)),
            pltpu.SemaphoreType.DMA((2 * number,)),
            pltpu.SemaphoreType.DMA((2 * number,)),
            pltpu.SemaphoreType.DMA((2 + groups,)),
            pltpu.SemaphoreType.DMA((2 + groups,)),
        ],
        compiler_params=pltpu.CompilerParams(
            collective_id=index, has_side_effects=True, vmem_limit_bytes=40 * 2**20
        ),
        name=f"exchange{index}",
    )(tab, potentials)


def lens_kernel(ratios, pot, h1, w, h, conv, shear, rot, disp):
    g = pl.program_id(0)
    rows = w.shape[1]
    columns = h1.shape[1]
    blocks = columns // LANES
    lane = iota((rows, LANES), 1)
    lane8 = iota((8, LANES), 1)
    sub = iota((8, LANES), 0)
    near_far, beta_one, beta_two = ratios[0], ratios[1], ratios[2]

    def across(x, t, k, where):
        ahead = pltpu.roll(jnp.where(where < k, t, x), LANES - k, 1)
        behind = pltpu.roll(jnp.where(where >= LANES - k, t, x), k, 1)
        return ahead, behind

    def slope_parts(x, t, where):
        a1, b1 = across(x, t, 1, where)
        a2, b2 = across(x, t, 2, where)
        return 8.0 * (a1 - b1) - (a2 - b2), a1 + b1, a2 + b2

    def second(x, s1, s2, s3, s4):
        return 16.0 * (s1 - s3) + 64.0 * s2 + s4 - 130.0 * x

    def along(a, b, e, k):
        plus = (
            pltpu.roll(jnp.where(sub < k, b, a), 8 - k, 0),
            pltpu.roll(jnp.where(sub < k, e, b), 8 - k, 0),
        )
        minus = (
            pltpu.roll(jnp.where(sub >= 8 - k, e, a), k, 0),
            pltpu.roll(jnp.where(sub >= 8 - k, a, b), k, 0),
        )
        return plus, minus

    def derive(x, t, e, te):
        slope_c, s1, s2 = slope_parts(x, t, lane)
        a3, b3 = across(x, t, 3, lane)
        a4, b4 = across(x, t, 4, lane)
        curve_cc = second(x, s1, s2, a3 + b3, a4 + b4)
        slope_c_e, _, _ = slope_parts(e, te, lane8)
        a, b = x[:8], x[8:]
        p1, m1 = along(a, b, e, 1)
        p2, m2 = along(a, b, e, 2)
        p3, m3 = along(a, b, e, 3)
        p4, m4 = along(a, b, e, 4)
        ca, cb = slope_c[:8], slope_c[8:]
        q1, n1 = along(ca, cb, slope_c_e, 1)
        q2, n2 = along(ca, cb, slope_c_e, 2)
        slope_r, curve_rr, curve_rc = [], [], []
        for i, mid in enumerate((a, b)):
            slope_r.append(8.0 * (p1[i] - m1[i]) - (p2[i] - m2[i]))
            curve_rr.append(second(mid, p1[i] + m1[i], p2[i] + m2[i], p3[i] + m3[i], p4[i] + m4[i]))
            curve_rc.append(8.0 * (q1[i] - n1[i]) - (q2[i] - n2[i]))
        join = functools.partial(jnp.concatenate, axis=0)
        return join(slope_r), slope_c, join(curve_rr), join(curve_rc), curve_cc

    one = 1.0 / 12.0
    two = 1.0 / 144.0
    for j in range(GROUP):
        c = g * GROUP + j
        before = lax.rem(c + (blocks - 1), blocks)
        after = lax.rem(c + 1, blocks)

        def at(i):
            return pl.ds(pl.multiple_of(i * LANES, LANES), LANES)

        near = derive(
            pot[0, :, at(c)],
            jnp.where(lane >= LANES // 2, pot[0, :, at(before)], pot[0, :, at(after)]),
            h1[:, at(c)],
            jnp.where(lane8 >= LANES // 2, h1[:, at(before)], h1[:, at(after)]),
        )
        back = (LANES - 8 * j - 4) % LANES
        far = derive(w[j], pltpu.roll(w[GROUP], back, 1), h[j], pltpu.roll(h[GROUP], back, 1))
        near_r, near_c, near_rr, near_rc, near_cc = near
        far_r, far_c, far_rr, far_rc, far_cc = far
        near_rr, near_rc, near_cc = near_rr * two, near_rc * two, near_cc * two
        inner_rr = 1.0 - near_far * near_rr
        inner_cc = 1.0 - near_far * near_cc
        inner_rc = -near_far * near_rc
        scale = 0.5 * two * beta_two
        half_one = 0.5 * beta_one
        chain_rr = far_rr * inner_rr + far_rc * inner_rc
        chain_cc = far_rc * inner_rc + far_cc * inner_cc
        chain_rc = far_rr * inner_rc + far_rc * inner_cc
        chain_cr = far_rc * inner_rr + far_cc * inner_rc
        spot = pl.ds(j * LANES, LANES)
        conv[:, spot] = half_one * (near_rr + near_cc) + scale * (chain_rr + chain_cc)
        shear[0, :, spot] = half_one * (near_cc - near_rr) + scale * (chain_cc - chain_rr)
        shear[1, :, spot] = beta_one * near_rc + scale * (chain_rc + chain_cr)
        rot[:, spot] = scale * (chain_cr - chain_rc)
        disp[0, :, spot] = (one * beta_one) * near_r + (one * beta_two) * far_r
        disp[1, :, spot] = (one * beta_one) * near_c + (one * beta_two) * far_c


def lens(ratios, potentials, h1, w, h):
    rows, columns = potentials.shape[1:]
    packet = GROUP + 1
    wide = GROUP * LANES
    f32 = jnp.float32
    flat = jax.ShapeDtypeStruct((rows, columns), f32)
    pair = jax.ShapeDtypeStruct((2, rows, columns), f32)
    flat_spec = pl.BlockSpec((rows, wide), lambda g: (0, g))
    pair_spec = pl.BlockSpec((2, rows, wide), lambda g: (0, 0, g))
    return pl.pallas_call(
        lens_kernel,
        grid=(columns // wide,),
        out_shape=(flat, pair, flat, pair),
        in_specs=[
            pl.BlockSpec(memory_space=pltpu.SMEM),
            pl.BlockSpec((1, rows, columns), lambda g: (0, 0, 0)),
            pl.BlockSpec((8, columns), lambda g: (0, 0)),
            pl.BlockSpec((packet, rows, LANES), lambda g: (g, 0, 0)),
            pl.BlockSpec((packet, 8, LANES), lambda g: (g, 0, 0)),
        ],
        out_specs=(flat_spec, pair_spec, flat_spec, pair_spec),
        compiler_params=pltpu.CompilerParams(vmem_limit_bytes=40 * 2**20),
        name="lens",
    )(ratios, potentials, h1, w, h)


def per_device(potentials, ratios, row_offset, col_offset):
    blocks = row_offset.shape[0]
    vmem = pl.BlockSpec(memory_space=pltpu.VMEM)
    tab = pl.pallas_call(
        table_kernel,
        out_shape=jax.ShapeDtypeStruct((8, blocks), jnp.int32),
        in_specs=[vmem, vmem],
        out_specs=vmem,
        name="table",
    )(row_offset.reshape(1, blocks), col_offset.reshape(1, blocks))
    w, h, h1 = lax.cond(
        tab[7, 0] == 0,
        functools.partial(exchange, 0),
        functools.partial(exchange, 1),
        tab,
        potentials,
    )
    return lens(ratios, potentials, h1, w, h)


def solution(mesh):
    return jax.shard_map(
        per_device,
        mesh=mesh,
        in_specs=(P("cosmo", "row", None), P("cosmo"), P("cosmo"), P("cosmo")),
        out_specs=(
            P(("cosmo", "row"), None),
            P(None, ("cosmo", "row"), None),
            P(("cosmo", "row"), None),
            P(None, ("cosmo", "row"), None),
        ),
        check_vma=False,
    )
```

```python
import functools

import jax
import jax.numpy as jnp
from jax import lax
from jax.experimental import pallas as pl
from jax.experimental.pallas import tpu as pltpu
from jax.sharding import PartitionSpec as P

RB = 8
LANES = 128
HALF = RB // 2
GROUP = 16
PACKET = GROUP + 1
EDGE = 4
MESH = pl.DeviceIdType.MESH

PLANS = (((4, 3, 2, 1), (3, 6, 8)), ((8, 8, 8, 4), (8,)))
STORES = ((0, 1), (2,), (3,))


def chunk_base(hops):
    base, total = [], 0
    for count in hops:
        base.append(total)
        total += count
    return base, total


def store_of(hop):
    return [i for i, members in enumerate(STORES) if hop in members][0]


def store_size(hops, i):
    return sum(hops[hop] for hop in STORES[i])


def store_base(hops, hop):
    members = STORES[store_of(hop)]
    return sum(hops[other] for other in members if other < hop)


def iota(shape, dim):
    return lax.broadcasted_iota(jnp.int32, shape, dim)


def table_kernel(row_ref, col_ref, tab_ref):
    blocks = row_ref.shape[1]
    square = (blocks, blocks)
    f32 = jnp.float32
    row = row_ref[...].astype(f32)
    lane_f = iota((1, blocks), 1).astype(f32)
    source = lane_f + col_ref[...].astype(f32)
    source = jnp.where(source >= blocks, source - blocks, source)
    sub2 = iota(square, 0)
    lane2 = iota(square, 1)
    lane2_f = lane2.astype(f32)

    def spread(v):
        return jnp.broadcast_to(v, square)

    def column(v):
        return spread(jnp.sum(jnp.where(sub2 == lane2, spread(v), 0.0), axis=1, keepdims=True))

    def total(v):
        return jnp.sum(v, axis=1, keepdims=True)

    def down(v):
        return jnp.sum(v, axis=0, keepdims=True)

    halfway = (row == HALF).astype(f32)
    dist = jnp.where(row <= HALF, row, RB - row)
    n_half = total(halfway)
    load_a = total(jnp.where(row < HALF, row, 0.0))
    load_b = total(jnp.where(row > HALF, RB - row, 0.0))
    take_a = jnp.clip(jnp.floor((load_b + HALF * n_half - load_a) / (2 * HALF) + 0.5), 0.0, n_half)
    rank_half = down(jnp.where(sub2 < lane2, column(halfway), 0.0))
    way = jnp.where(row == 0, 0.0, jnp.where(row < HALF, 1.0, 2.0))
    way = jnp.where((row == HALF) & (rank_half < take_a), 1.0, way)
    big = 4096.0
    key = way * big + (HALF - dist) * blocks + lane_f
    key_c = column(key)
    slot = down(((key_c < spread(key)) & (key_c >= spread(way * big))).astype(f32))
    near = dist * blocks + lane_f
    near_c = column(near)
    place = down((near_c < spread(near)).astype(f32))

    fits = jnp.ones((1, 1), f32)
    hops, ends = PLANS[0]
    for hop, count in enumerate(hops):
        for w in (1.0, 2.0):
            need = total(((way == w) & (dist > hop)).astype(f32))
            fits = jnp.where(need > count * GROUP, 0.0, fits)
    for end, reach in zip(ends, (2, 3, 4)):
        fits = jnp.where(total((dist <= reach).astype(f32)) < end * GROUP, 0.0, fits)
    fits = jnp.where(total((dist == 0).astype(f32)) > ends[0] * GROUP, 0.0, fits)

    chunk = jnp.floor(slot / GROUP)
    within = slot - chunk * GROUP
    spot = []
    for hops, _ in PLANS:
        at = jnp.zeros((1, blocks), f32)
        for hop in range(HALF):
            other = jnp.where(way == 2.0, float(store_size(hops, store_of(hop))), 0.0)
            at = jnp.where(dist == hop + 1, other + float(store_base(hops, hop)), at)
        spot.append(at + chunk)
    spot = jnp.where(fits > 0, spot[0], spot[1])
    spot = jnp.where(way == 0, 0.0, spot)
    within = jnp.where(way == 0, 0.0, within)
    kind = jnp.zeros((1, blocks), f32)
    for hop in range(HALF):
        kind = jnp.where(dist == hop + 1, float(store_of(hop) + 1), kind)

    slot_c, way_c, source_c, place_c = column(slot), column(way), column(source), column(place)
    here = slot_c == lane2_f
    send = [down(jnp.where(here & (way_c == w), source_c, 0.0)) for w in (1.0, 2.0)]
    there = place_c == lane2_f

    def ordered(v):
        return down(jnp.where(there, column(v), 0.0))

    at = ordered(spot)
    inside = ordered(within)
    turn = 8.0 * (lane_f - GROUP * jnp.floor(lane_f / GROUP) - inside)
    turn = jnp.where(turn < 0, turn + LANES, turn)
    rows = [
        send[0],
        send[1],
        at * PACKET + inside,
        at * PACKET + GROUP,
        turn,
        down(jnp.where(there, source_c, 0.0)),
        ordered(kind),
        down(jnp.where(there, sub2.astype(f32), 0.0)),
        place,
        spread(1.0 - fits)[:1],
    ]
    rows += [jnp.zeros((1, blocks), f32)] * (16 - len(rows))
    tab_ref[...] = jnp.concatenate(rows, axis=0).astype(jnp.int32)


def exchange_kernel(plan, tab, ratios, pot, out, p1, p2, tiles, sent, got_a, got_b, got_c, v1, v2, near, c1s, ccs,
                    local_sem, send_sem, recv_sem, edge_send, edge_recv):
    hops, ends = plan
    base, number = chunk_base(hops)
    stores = (got_a, got_b, got_c)
    size = lax.axis_size("row")
    stride = size // RB
    me = lax.axis_index("row")
    blocks = tiles.shape[0]
    rows = tiles.shape[1]
    tall = rows + 2 * EDGE
    first = hops[0]
    single = len(ends) == 1

    load2 = pltpu.make_async_copy(pot.at[1], p2, local_sem.at[0])
    load1 = pltpu.make_async_copy(pot.at[0], p1, local_sem.at[1])
    load2.start()
    load1.start()
    barrier = pltpu.get_barrier_semaphore()
    for by in (stride, size - stride, 1, size - 1):
        pl.semaphore_signal(barrier, inc=1, device_id={"row": lax.rem(me + by, size)}, device_id_type=MESH)

    lane = iota((rows, LANES), 1)
    lane_group = lane // 8
    lane_t = iota((tall, LANES), 1)

    def split(source, put):
        def body(i, carry):
            for j in range(GROUP):
                b = i * GROUP + j
                put(b, source[:, pl.ds(pl.multiple_of(b * LANES, LANES), LANES)])
            return carry

        lax.fori_loop(0, blocks // GROUP, body, 0)

    def put_tile(b, value):
        tiles[b] = value

    def put_v1(b, value):
        v1[b, EDGE : EDGE + rows, :] = value

    def sides(s):
        before = tiles[lax.rem(s + (blocks - 1), blocks)]
        after = tiles[lax.rem(s + 1, blocks)]
        return jnp.where(lane >= LANES // 2, before, after)

    def pack(i):
        way = lax.rem(i, 2)
        chunk = i // 2
        halo = jnp.zeros((rows, LANES), jnp.float32)
        for j in range(GROUP):
            s = tab[way, chunk * GROUP + j]
            sent[i * PACKET + j] = tiles[s]
            halo = jnp.where(lane_group == j, pltpu.roll(sides(s), (8 * j + 4) % LANES, 1), halo)
        sent[i * PACKET + GROUP] = halo

    def first_copy(i):
        way = lax.rem(i, 2)
        to = way * number + i // 2
        land = way * store_size(hops, 0) + i // 2
        return pltpu.make_async_remote_copy(
            src_ref=sent.at[pl.ds(i * PACKET, PACKET)],
            dst_ref=got_a.at[pl.ds(land * PACKET, PACKET)],
            send_sem=send_sem.at[to],
            recv_sem=recv_sem.at[to],
            device_id={"row": lax.rem(me + jnp.where(way == 0, size - stride, stride), size)},
            device_id_type=MESH,
        )

    def piece(way, hop, c):
        where = store_of(hop)
        at = way * store_size(hops, where) + store_base(hops, hop) + c
        return stores[where].at[pl.ds(at * PACKET, PACKET)]

    def relay(way, hop, c):
        to = way * number + base[hop] + c
        return pltpu.make_async_remote_copy(
            src_ref=piece(way, hop - 1, c),
            dst_ref=piece(way, hop, c),
            send_sem=send_sem.at[to],
            recv_sem=recv_sem.at[to],
            device_id={"row": lax.rem(me + (size - stride if way == 0 else stride), size)},
            device_id_type=MESH,
        )

    def arrival(way, hop, c):
        to = way * number + base[hop] + c
        here = piece(way, hop, c)
        return pltpu.make_async_remote_copy(
            src_ref=here, dst_ref=here, send_sem=send_sem.at[to], recv_sem=recv_sem.at[to],
            device_id={"row": lax.rem(me + stride, size)}, device_id_type=MESH,
        )

    def edges(ref, begin, end, at):
        span = pl.ds(begin, end - begin)
        pair = []
        for k, (src, dst, by) in enumerate(((rows, 0, 1), (EDGE, EDGE + rows, size - 1))):
            pair.append(
                pltpu.make_async_remote_copy(
                    src_ref=ref.at[span, src : src + EDGE, :],
                    dst_ref=ref.at[span, dst : dst + EDGE, :],
                    send_sem=edge_send.at[2 * at + k],
                    recv_sem=edge_recv.at[2 * at + k],
                    device_id={"row": lax.rem(me + by, size)},
                    device_id_type=MESH,
                )
            )
        return pair

    load2.wait()
    split(p2, put_tile)
    pack(0)
    pl.semaphore_wait(barrier, 4)

    def step(i, carry):
        pack(i)
        first_copy(i - 1).start()
        return carry

    lax.fori_loop(1, 2 * first, step, 0)
    first_copy(2 * first - 1).start()

    load1.wait()
    split(p1, put_v1)
    edges1 = edges(v1, 0, blocks, 0)
    for copy in edges1:
        copy.start()

    near_far, beta_one, beta_two = ratios[0], ratios[1], ratios[2]
    one = 1.0 / 12.0
    two = 1.0 / 144.0

    def second(x, s1, s2, s3, s4):
        return 16.0 * (s1 - s3) + 64.0 * s2 + s4 - 130.0 * x

    def derive(ref, f, t, j):
        x = ref[f]
        ahead = [pltpu.roll(jnp.where(lane_t < k, t, x), LANES - k, 1) for k in range(1, 5)]
        behind = [pltpu.roll(jnp.where(lane_t >= LANES - k, t, x), k, 1) for k in range(1, 5)]
        c1s[j] = 8.0 * (ahead[0] - behind[0]) - (ahead[1] - behind[1])
        ccs[j] = second(x, *[a + b for a, b in zip(ahead, behind)])

        def tap(k):
            return ref[f, EDGE + k : EDGE + k + rows, :]

        def tap_c(k):
            return c1s[j, EDGE + k : EDGE + k + rows, :]

        up = [tap(k) for k in range(1, 5)]
        low = [tap(-k) for k in range(1, 5)]
        slope_r = 8.0 * (up[0] - low[0]) - (up[1] - low[1])
        curve_rr = second(tap(0), *[a + b for a, b in zip(up, low)])
        curve_rc = 8.0 * (tap_c(1) - tap_c(-1)) - (tap_c(2) - tap_c(-2))
        curve_cc = ccs[j, EDGE : EDGE + rows, :]
        return slope_r, tap_c(0), curve_rr, curve_rc, curve_cc

    def near_group(g):
        for j in range(GROUP):
            b = g * GROUP + j
            before = v1[lax.rem(b + (blocks - 1), blocks)]
            after = v1[lax.rem(b + 1, blocks)]
            slope_r, slope_c, curve_rr, curve_rc, curve_cc = derive(v1, b, jnp.where(lane_t >= LANES // 2, before, after), j)
            near[b, 0 * rows : 1 * rows, :] = two * (curve_rr + curve_cc)
            near[b, 1 * rows : 2 * rows, :] = two * (curve_cc - curve_rr)
            near[b, 2 * rows : 3 * rows, :] = (2.0 * two) * curve_rc
            near[b, 3 * rows : 4 * rows, :] = (one * beta_one) * slope_r
            near[b, 4 * rows : 5 * rows, :] = (one * beta_one) * slope_c

    def near_groups(begin, end):
        def body(g, carry):
            near_group(g)
            return carry

        lax.fori_loop(begin, end, body, 0)

    def gather(begin, end, kinds):
        def body(g, carry):
            halo = jnp.zeros((rows, LANES), jnp.float32)
            for j in range(GROUP):
                f = g * GROUP + j
                kind = jnp.full((rows, LANES), tab[6, f], jnp.int32)
                value = cols = None
                for k in kinds:
                    if k == 0:
                        s = tab[5, f]
                        v, c = tiles[s], pltpu.roll(sides(s), (8 * j + 4) % LANES, 1)
                    else:
                        ref = stores[k - 1]
                        limit = ref.shape[0] - 1
                        v = ref[jnp.minimum(tab[2, f], limit)]
                        c = ref[jnp.minimum(tab[3, f], limit)]
                        c = pltpu.roll(c, tab[4, f], 1)
                    value = v if value is None else jnp.where(kind == k, v, value)
                    cols = c if cols is None else jnp.where(kind == k, c, cols)
                halo = jnp.where(lane_group == j, cols, halo)
                v2[g * PACKET + j, EDGE : EDGE + rows, :] = value
            v2[g * PACKET + GROUP, EDGE : EDGE + rows, :] = halo
            return carry

        lax.fori_loop(begin, end, body, 0)

    scale = 0.5 * two * beta_two
    half_far = 0.5 * near_far
    half_one = 0.5 * beta_one
    slope_scale = one * beta_two

    def combine(begin, end):
        def body(g, carry):
            halo = v2[g * PACKET + GROUP]
            for j in range(GROUP):
                f = g * GROUP + j
                t = pltpu.roll(halo, (LANES - 8 * j - 4) % LANES, 1)
                far_r, far_c, far_rr, far_rc, far_cc = derive(v2, g * PACKET + j, t, j)
                n = near[tab[7, f]]
                n_sum, n_diff, n_rc2, n_r, n_c = (n[k * rows : (k + 1) * rows] for k in range(5))
                s = scale * (far_rr + far_cc)
                d = scale * (far_cc - far_rr)
                r = scale * far_rc
                d_half = half_far * d
                r_far = near_far * r
                rest = half_one - half_far * s
                out[f, 0 * rows : 1 * rows, :] = s + n_sum * rest - d_half * n_diff - r_far * n_rc2
                out[f, 1 * rows : 2 * rows, :] = d + n_diff * rest - d_half * n_sum
                out[f, 2 * rows : 3 * rows, :] = (r + r) + n_rc2 * rest - r_far * n_sum
                out[f, 3 * rows : 4 * rows, :] = r_far * n_diff - n_rc2 * d_half
                out[f, 4 * rows : 5 * rows, :] = n_r + slope_scale * far_r
                out[f, 5 * rows : 6 * rows, :] = n_c + slope_scale * far_c
            return carry

        lax.fori_loop(begin, end, body, 0)

    def forward(hop, c):
        for way in range(2):
            arrival(way, hop - 1, c).wait_recv()
            relay(way, hop, c).start()

    def land(hop):
        for c in range(hops[hop + 1] if hop + 1 < HALF else 0, hops[hop]):
            for way in range(2):
                arrival(way, hop, c).wait_recv()

    groups = blocks // GROUP
    relays = [(hop, c) for hop in range(1, HALF) for c in range(hops[hop])]
    late = [(hop, c) for hop, c in relays if hop == HALF - 1]
    early = [pair for pair in relays if pair not in late]
    share = max(1, -(-groups // (len(early) - 1)))
    done = 0
    for i, (hop, c) in enumerate(early):
        forward(hop, c)
        if i == 0:
            for copy in edges1:
                copy.wait_recv()
        upto = min(groups, done + share)
        if upto > done:
            near_groups(done, upto)
        done = upto
    if done < groups:
        near_groups(done, groups)

    bounds = [0] + list(ends)
    moved = [edges(v2, bounds[p] * PACKET, bounds[p + 1] * PACKET, 1 + p) for p in range(len(ends))]

    def begin_phase(p, kinds):
        gather(bounds[p], bounds[p + 1], kinds)
        for copy in moved[p]:
            copy.start()

    def end_phase(p):
        for copy in moved[p]:
            copy.wait_recv()
        combine(bounds[p], bounds[p + 1])

    land(0)
    land(1)
    if single:
        for hop, c in late:
            forward(hop, c)
        land(2)
        land(3)
        begin_phase(0, (0, 1, 2, 3))
        end_phase(0)
    else:
        begin_phase(0, (0, 1))
        for hop, c in late:
            forward(hop, c)
        end_phase(0)
        land(2)
        begin_phase(1, (1, 2))
        land(3)
        begin_phase(2, (1, 2, 3))
        end_phase(1)
        end_phase(2)

    for copy in edges1:
        copy.wait_send()
    for pair in moved:
        for copy in pair:
            copy.wait_send()
    for way in range(2):
        for hop in range(HALF):
            for c in range(hops[hop]):
                arrival(way, hop, c).wait_send()


def exchange(index, tab, ratios, potentials):
    plan = PLANS[index]
    hops, ends = plan
    rows, columns = potentials.shape[1:]
    blocks = columns // LANES
    _, number = chunk_base(hops)
    packets = blocks // GROUP * PACKET
    tall = rows + 2 * EDGE
    f32 = jnp.float32
    smem = pl.BlockSpec(memory_space=pltpu.SMEM)
    return pl.pallas_call(
        functools.partial(exchange_kernel, plan),
        out_shape=jax.ShapeDtypeStruct((blocks, 6 * rows, LANES), f32),
        in_specs=[smem, smem, pl.BlockSpec(memory_space=pl.ANY)],
        out_specs=pl.BlockSpec(memory_space=pltpu.VMEM),
        scratch_shapes=[
            pltpu.VMEM((rows, columns), f32),
            pltpu.VMEM((rows, columns), f32),
            pltpu.VMEM((blocks, rows, LANES), f32),
            pltpu.VMEM((2 * hops[0] * PACKET, rows, LANES), f32),
            *[pltpu.VMEM((2 * store_size(hops, i) * PACKET, rows, LANES), f32) for i in range(len(STORES))],
            pltpu.VMEM((blocks, tall, LANES), f32),
            pltpu.VMEM((packets, tall, LANES), f32),
            pltpu.VMEM((blocks, 5 * rows, LANES), f32),
            pltpu.VMEM((GROUP, tall, LANES), f32),
            pltpu.VMEM((GROUP, tall, LANES), f32),
            pltpu.SemaphoreType.DMA((2,)),
            pltpu.SemaphoreType.DMA((2 * number,)),
            pltpu.SemaphoreType.DMA((2 * number,)),
            pltpu.SemaphoreType.DMA((2 + 2 * len(ends),)),
            pltpu.SemaphoreType.DMA((2 + 2 * len(ends),)),
        ],
        compiler_params=pltpu.CompilerParams(
            collective_id=index, has_side_effects=True, vmem_limit_bytes=30 * 2**20
        ),
        name=f"exchange{index}",
    )(tab, ratios, potentials)


def arrange_kernel(tab, fields, conv, shear, rot, disp):
    g = pl.program_id(0)
    rows = conv.shape[0]
    for j in range(GROUP):
        value = fields[tab[8, g * GROUP + j]]
        part = [value[k * rows : (k + 1) * rows] for k in range(6)]
        spot = slice(j * LANES, (j + 1) * LANES)
        conv[:, spot] = part[0]
        shear[0, :, spot] = part[1]
        shear[1, :, spot] = part[2]
        rot[:, spot] = part[3]
        disp[0, :, spot] = part[4]
        disp[1, :, spot] = part[5]


def arrange(tab, fields, rows):
    columns = fields.shape[0] * LANES
    wide = GROUP * LANES
    f32 = jnp.float32
    flat = jax.ShapeDtypeStruct((rows, columns), f32)
    pair = jax.ShapeDtypeStruct((2, rows, columns), f32)
    flat_spec = pl.BlockSpec((rows, wide), lambda g: (0, g))
    pair_spec = pl.BlockSpec((2, rows, wide), lambda g: (0, 0, g))
    return pl.pallas_call(
        arrange_kernel,
        grid=(columns // wide,),
        out_shape=(flat, pair, flat, pair),
        in_specs=[pl.BlockSpec(memory_space=pltpu.SMEM), pl.BlockSpec(memory_space=pltpu.VMEM)],
        out_specs=(flat_spec, pair_spec, flat_spec, pair_spec),
        compiler_params=pltpu.CompilerParams(vmem_limit_bytes=16 * 2**20),
        name="arrange",
    )(tab, fields)


def per_device(potentials, ratios, row_offset, col_offset):
    blocks = row_offset.shape[0]
    vmem = pl.BlockSpec(memory_space=pltpu.VMEM)
    tab = pl.pallas_call(
        table_kernel,
        out_shape=jax.ShapeDtypeStruct((16, blocks), jnp.int32),
        in_specs=[vmem, vmem],
        out_specs=vmem,
        compiler_params=pltpu.CompilerParams(vmem_limit_bytes=4 * 2**20),
        name="table",
    )(row_offset.reshape(1, blocks), col_offset.reshape(1, blocks))
    def run(index, tab, ratios, potentials):
        return arrange(tab, exchange(index, tab, ratios, potentials), potentials.shape[1])

    return lax.cond(
        tab[9, 0] == 0, functools.partial(run, 0), functools.partial(run, 1), tab, ratios, potentials
    )


def solution(mesh):
    return jax.shard_map(
        per_device,
        mesh=mesh,
        in_specs=(P("cosmo", "row", None), P("cosmo"), P("cosmo"), P("cosmo")),
        out_specs=(
            P(("cosmo", "row"), None),
            P(None, ("cosmo", "row"), None),
            P(("cosmo", "row"), None),
            P(None, ("cosmo", "row"), None),
        ),
        check_vma=False,
    )
```

```python
import functools

import jax
import jax.numpy as jnp
from jax import lax
from jax.experimental import pallas as pl
from jax.experimental.pallas import tpu as pltpu
from jax.sharding import PartitionSpec as P

RB = 8
LANES = 128
HALF = RB // 2
GROUP = 16
PACKET = GROUP + 1
EDGE = 4
MESH = pl.DeviceIdType.MESH

PLANS = (
    ((4, 3, 2, 1), ((2, 0, 1), (4, 1, 2), (6, 2, 3), (8, 3, 4))),
    ((4, 3, 2, 1), ((3, 0, 2), (6, 1, 3), (8, 2, 4))),
    ((8, 8, 8, 4), ((8, 0, 4),)),
)
STORES = ((0,), (1,), (2,), (3,))


def chunk_base(hops):
    base, total = [], 0
    for count in hops:
        base.append(total)
        total += count
    return base, total


def store_of(hop):
    return [i for i, members in enumerate(STORES) if hop in members][0]


def store_size(hops, i):
    return sum(hops[hop] for hop in STORES[i])


def store_base(hops, hop):
    members = STORES[store_of(hop)]
    return sum(hops[other] for other in members if other < hop)


def iota(shape, dim):
    return lax.broadcasted_iota(jnp.int32, shape, dim)


def table_kernel(row_ref, col_ref, tab_ref):
    blocks = row_ref.shape[1]
    square = (blocks, blocks)
    f32 = jnp.float32
    row = row_ref[...].astype(f32)
    lane_f = iota((1, blocks), 1).astype(f32)
    source = lane_f + col_ref[...].astype(f32)
    source = jnp.where(source >= blocks, source - blocks, source)
    sub2 = iota(square, 0)
    lane2 = iota(square, 1)
    lane2_f = lane2.astype(f32)

    def spread(v):
        return jnp.broadcast_to(v, square)

    def column(v):
        return spread(jnp.sum(jnp.where(sub2 == lane2, spread(v), 0.0), axis=1, keepdims=True))

    def total(v):
        return jnp.sum(v, axis=1, keepdims=True)

    def down(v):
        return jnp.sum(v, axis=0, keepdims=True)

    halfway = (row == HALF).astype(f32)
    dist = jnp.where(row <= HALF, row, RB - row)
    n_half = total(halfway)
    load_a = total(jnp.where(row < HALF, row, 0.0))
    load_b = total(jnp.where(row > HALF, RB - row, 0.0))
    take_a = jnp.clip(jnp.floor((load_b + HALF * n_half - load_a) / (2 * HALF) + 0.5), 0.0, n_half)
    rank_half = down(jnp.where(sub2 < lane2, column(halfway), 0.0))
    way = jnp.where(row == 0, 0.0, jnp.where(row < HALF, 1.0, 2.0))
    way = jnp.where((row == HALF) & (rank_half < take_a), 1.0, way)
    big = 4096.0
    key = way * big + (HALF - dist) * blocks + lane_f
    key_c = column(key)
    slot = down(((key_c < spread(key)) & (key_c >= spread(way * big))).astype(f32))
    near = dist * blocks + lane_f
    near_c = column(near)
    place = down((near_c < spread(near)).astype(f32))

    def fitting(plan):
        hops, phases = plan
        fits = jnp.ones((1, 1), f32)
        for hop, count in enumerate(hops):
            for w in (1.0, 2.0):
                fits = jnp.where(total(((way == w) & (dist > hop)).astype(f32)) > count * GROUP, 0.0, fits)
        start = 0
        for end, least, reach in phases:
            fits = jnp.where(total((dist < least).astype(f32)) > start * GROUP, 0.0, fits)
            fits = jnp.where(total((dist <= reach).astype(f32)) < end * GROUP, 0.0, fits)
            start = end
        return fits

    fits = [fitting(plan) for plan in PLANS[:-1]]
    choice = jnp.full((1, 1), float(len(PLANS) - 1), f32)
    for i in reversed(range(len(PLANS) - 1)):
        choice = jnp.where(fits[i] > 0, float(i), choice)

    chunk = jnp.floor(slot / GROUP)
    within = slot - chunk * GROUP
    spot = []
    for hops, _ in PLANS:
        at = jnp.zeros((1, blocks), f32)
        for hop in range(HALF):
            other = jnp.where(way == 2.0, float(store_size(hops, store_of(hop))), 0.0)
            at = jnp.where(dist == hop + 1, other + float(store_base(hops, hop)), at)
        spot.append(at + chunk)
    spot = functools.reduce(lambda rest, i: jnp.where(choice == i, spot[i], rest), range(len(PLANS) - 1), spot[-1])
    spot = jnp.where(way == 0, 0.0, spot)
    within = jnp.where(way == 0, 0.0, within)
    slot_c, way_c, source_c, place_c = column(slot), column(way), column(source), column(place)
    here = slot_c == lane2_f
    send = [down(jnp.where(here & (way_c == w), source_c, 0.0)) for w in (1.0, 2.0)]
    there = place_c == lane2_f

    def ordered(v):
        return down(jnp.where(there, column(v), 0.0))

    at = ordered(spot)
    inside = ordered(within)
    kind = ordered(dist)
    turn = 8.0 * (lane_f - GROUP * jnp.floor(lane_f / GROUP) - inside) + jnp.where(kind == 0, 4.0, 0.0)
    turn = jnp.where(turn < 0, turn + LANES, turn)
    rows = [
        send[0],
        send[1],
        at * PACKET + inside,
        at * PACKET + GROUP,
        turn,
        down(jnp.where(there, source_c, 0.0)),
        kind,
        down(jnp.where(there, sub2.astype(f32), 0.0)),
        place,
        spread(choice)[:1],
    ]
    rows += [jnp.zeros((1, blocks), f32)] * (16 - len(rows))
    tab_ref[...] = jnp.concatenate(rows, axis=0).astype(jnp.int32)


def exchange_kernel(plan, tab, ratios, pot, out, p1, p2, tiles, sent, got_a, got_b, got_c, got_d, v1, v2, near, c1s,
                    local_sem, send_sem, recv_sem, edge_send, edge_recv):
    hops, phases = plan
    base, number = chunk_base(hops)
    stores = (got_a, got_b, got_c, got_d)
    size = lax.axis_size("row")
    stride = size // RB
    me = lax.axis_index("row")
    blocks = tiles.shape[0]
    rows = tiles.shape[1]
    tall = rows + 2 * EDGE
    first = hops[0]

    load2 = pltpu.make_async_copy(pot.at[1], p2, local_sem.at[0])
    load1 = pltpu.make_async_copy(pot.at[0], p1, local_sem.at[1])
    load2.start()
    load1.start()
    barrier = pltpu.get_barrier_semaphore()
    for by in (stride, size - stride, 1, size - 1):
        pl.semaphore_signal(barrier, inc=1, device_id={"row": lax.rem(me + by, size)}, device_id_type=MESH)

    lane = iota((rows, LANES), 1)
    lane_group = lane // 8

    def split(source, put):
        def body(i, carry):
            for j in range(GROUP):
                b = i * GROUP + j
                put(b, source[:, pl.ds(pl.multiple_of(b * LANES, LANES), LANES)])
            return carry

        lax.fori_loop(0, blocks // GROUP, body, 0)

    def put_tile(b, value):
        tiles[b] = value

    def put_v1(b, value):
        v1[b, EDGE : EDGE + rows, :] = value

    def sides(s):
        before = tiles[(s + (blocks - 1)) & (blocks - 1)]
        after = tiles[(s + 1) & (blocks - 1)]
        return jnp.where(lane >= LANES // 2, before, after)

    def pack(i):
        way = lax.rem(i, 2)
        chunk = i // 2
        halo = jnp.zeros((rows, LANES), jnp.float32)
        for j in range(GROUP):
            s = tab[way, chunk * GROUP + j]
            sent[i * PACKET + j] = tiles[s]
            halo = jnp.where(lane_group == j, pltpu.roll(sides(s), (8 * j + 4) % LANES, 1), halo)
        sent[i * PACKET + GROUP] = halo

    def first_copy(i):
        way = lax.rem(i, 2)
        to = way * number + i // 2
        land = way * store_size(hops, 0) + i // 2
        return pltpu.make_async_remote_copy(
            src_ref=sent.at[pl.ds(i * PACKET, PACKET)],
            dst_ref=got_a.at[pl.ds(land * PACKET, PACKET)],
            send_sem=send_sem.at[to],
            recv_sem=recv_sem.at[to],
            device_id={"row": lax.rem(me + jnp.where(way == 0, size - stride, stride), size)},
            device_id_type=MESH,
        )

    def piece(way, hop, c):
        where = store_of(hop)
        at = way * store_size(hops, where) + store_base(hops, hop) + c
        return stores[where].at[pl.ds(at * PACKET, PACKET)]

    def relay(way, hop, c):
        to = way * number + base[hop] + c
        return pltpu.make_async_remote_copy(
            src_ref=piece(way, hop - 1, c),
            dst_ref=piece(way, hop, c),
            send_sem=send_sem.at[to],
            recv_sem=recv_sem.at[to],
            device_id={"row": lax.rem(me + (size - stride if way == 0 else stride), size)},
            device_id_type=MESH,
        )

    def arrival(way, hop, c):
        to = way * number + base[hop] + c
        here = piece(way, hop, c)
        return pltpu.make_async_remote_copy(
            src_ref=here, dst_ref=here, send_sem=send_sem.at[to], recv_sem=recv_sem.at[to],
            device_id={"row": lax.rem(me + stride, size)}, device_id_type=MESH,
        )

    def edges(ref, begin, end, at):
        span = pl.ds(begin, end - begin)
        pair = []
        for k, (src, dst, by) in enumerate(((rows, 0, 1), (EDGE, EDGE + rows, size - 1))):
            pair.append(
                pltpu.make_async_remote_copy(
                    src_ref=ref.at[span, src : src + EDGE, :],
                    dst_ref=ref.at[span, dst : dst + EDGE, :],
                    send_sem=edge_send.at[2 * at + k],
                    recv_sem=edge_recv.at[2 * at + k],
                    device_id={"row": lax.rem(me + by, size)},
                    device_id_type=MESH,
                )
            )
        return pair

    load2.wait()
    split(p2, put_tile)
    pack(0)
    pl.semaphore_wait(barrier, 4)

    def step(i, carry):
        pack(i)
        first_copy(i - 1).start()
        return carry

    lax.fori_loop(1, 2 * first, step, 0)
    first_copy(2 * first - 1).start()

    load1.wait()
    split(p1, put_v1)
    edges1 = edges(v1, 0, blocks, 0)
    for copy in edges1:
        copy.start()

    near_far, beta_one, beta_two = ratios[0], ratios[1], ratios[2]
    one = 1.0 / 12.0
    two = 1.0 / 144.0

    def second(x, s1, s2, s3, s4):
        return 16.0 * (s1 - s3) + 64.0 * s2 + s4 - 130.0 * x

    sub = iota((8, LANES), 0)
    lane8 = iota((8, LANES), 1)
    eight = rows // 2

    def thirds(ref, f):
        even = ref[f, pl.ds(EDGE, eight, stride=2), :]
        odd = ref[f, pl.ds(EDGE + 1, eight, stride=2), :]
        return even, odd, jnp.where(sub < EDGE, ref[f, 0:8, :], ref[f, tall - 8 : tall, :])

    def derive(ref, f, t, j):
        x = thirds(ref, f)

        def ahead(p, k):
            return pltpu.roll(jnp.where(lane8 < k, t[p], x[p]), LANES - k, 1)

        def behind(p, k):
            return pltpu.roll(jnp.where(lane8 >= LANES - k, t[p], x[p]), k, 1)

        slope_c, curve_cc = [], []
        for p in range(3):
            a1, b1, a2, b2 = ahead(p, 1), behind(p, 1), ahead(p, 2), behind(p, 2)
            slope_c.append(8.0 * (a1 - b1) - (a2 - b2))
            if p < 2:
                curve_cc.append(second(x[p], a1 + b1, a2 + b2, ahead(p, 3) + behind(p, 3), ahead(p, 4) + behind(p, 4)))
        for p in range(2):
            c1s[j, pl.ds(EDGE + p, eight, stride=2), :] = slope_c[p]
        c1s[j, 0:EDGE, :] = slope_c[2][:EDGE]
        c1s[j, tall - EDGE : tall, :] = slope_c[2][EDGE:]
        c = {EDGE: slope_c[0], EDGE + 1: slope_c[1]}
        r = {EDGE: x[0], EDGE + 1: x[1]}
        for at in (2, 3, 6, 7):
            c[at] = c1s[j, pl.ds(at, eight, stride=2), :]
        for at in (0, 1, 2, 3, 6, 7, 8, 9):
            r[at] = ref[f, pl.ds(at, eight, stride=2), :]
        slope_r, curve_rr, curve_rc = [], [], []
        for p in range(2):
            m = EDGE + p
            slope_r.append(8.0 * (r[m + 1] - r[m - 1]) - (r[m + 2] - r[m - 2]))
            curve_rr.append(second(r[m], *[r[m + k] + r[m - k] for k in range(1, 5)]))
            curve_rc.append(8.0 * (c[m + 1] - c[m - 1]) - (c[m + 2] - c[m - 2]))
        return slope_r, slope_c, curve_rr, curve_rc, curve_cc

    def near_group(g):
        for j in range(GROUP):
            b = g * GROUP + j
            before = thirds(v1, b - 1 if j > 0 else lax.rem(b + (blocks - 1), blocks))
            after = thirds(v1, b + 1 if j < GROUP - 1 else lax.rem(b + 1, blocks))
            t = [jnp.where(lane8 >= LANES // 2, before[p], after[p]) for p in range(3)]
            slope_r, slope_c, curve_rr, curve_rc, curve_cc = derive(v1, b, t, j)
            for p in range(2):
                values = (
                    two * (curve_rr[p] + curve_cc[p]),
                    two * (curve_cc[p] - curve_rr[p]),
                    (2.0 * two) * curve_rc[p],
                    (one * beta_one) * slope_r[p],
                    (one * beta_one) * slope_c[p],
                )
                for k, value in enumerate(values):
                    near[b, k * rows + p * eight : k * rows + (p + 1) * eight, :] = value

    def near_groups(begin, end):
        def body(g, carry):
            near_group(g)
            return carry

        lax.fori_loop(begin, end, body, 0)

    def gather(begin, end, kinds):
        def body(g, carry):
            halo = jnp.zeros((rows, LANES), jnp.float32)
            for j in range(GROUP):
                f = g * GROUP + j
                kind = jnp.full((rows, LANES), tab[6, f], jnp.int32)
                value = cols = None
                for k in kinds:
                    if k == 0:
                        s = tab[5, f]
                        v, c = tiles[s], sides(s)
                    else:
                        ref = stores[k - 1]
                        at_v, at_c = tab[2, f], tab[3, f]
                        if any(k2 > 0 and stores[k2 - 1].shape[0] > ref.shape[0] for k2 in kinds):
                            at_v, at_c = jnp.minimum(at_v, ref.shape[0] - 1), jnp.minimum(at_c, ref.shape[0] - 1)
                        v, c = ref[at_v], ref[at_c]
                    value = v if value is None else jnp.where(kind == k, v, value)
                    cols = c if cols is None else jnp.where(kind == k, c, cols)
                halo = jnp.where(lane_group == j, pltpu.roll(cols, tab[4, f], 1), halo)
                v2[g * PACKET + j, EDGE : EDGE + rows, :] = value
            v2[g * PACKET + GROUP, EDGE : EDGE + rows, :] = halo
            return carry

        lax.fori_loop(begin, end, body, 0)

    scale = 0.5 * two * beta_two
    half_far = 0.5 * near_far
    half_one = 0.5 * beta_one
    slope_scale = one * beta_two

    def combine(begin, end):
        def body(g, carry):
            halo = thirds(v2, g * PACKET + GROUP)
            for j in range(GROUP):
                f = g * GROUP + j
                t = [pltpu.roll(h, (LANES - 8 * j - 4) % LANES, 1) for h in halo]
                far_r, far_c, far_rr, far_rc, far_cc = derive(v2, g * PACKET + j, t, j)
                n = near[tab[7, f]]
                for p in range(2):
                    n_sum, n_diff, n_rc2, n_r, n_c = (
                        n[k * rows + p * eight : k * rows + (p + 1) * eight] for k in range(5)
                    )
                    s = scale * (far_rr[p] + far_cc[p])
                    d = scale * (far_cc[p] - far_rr[p])
                    r = scale * far_rc[p]
                    d_half = half_far * d
                    r_far = near_far * r
                    rest = half_one - half_far * s
                    results = (
                        s + n_sum * rest - d_half * n_diff - r_far * n_rc2,
                        d + n_diff * rest - d_half * n_sum,
                        (r + r) + n_rc2 * rest - r_far * n_sum,
                        r_far * n_diff - n_rc2 * d_half,
                        n_r + slope_scale * far_r[p],
                        n_c + slope_scale * far_c[p],
                    )
                    for k, value in enumerate(results):
                        out[f, pl.ds(k * rows + p, eight, stride=2), :] = value
            return carry

        lax.fori_loop(begin, end, body, 0)

    def forward(hop, c):
        for way in range(2):
            arrival(way, hop - 1, c).wait_recv()
            relay(way, hop, c).start()

    def land(hop):
        for c in range(hops[hop + 1] if hop + 1 < HALF else 0, hops[hop]):
            for way in range(2):
                arrival(way, hop, c).wait_recv()

    groups = blocks // GROUP
    bounds = [0] + [end for end, _, _ in phases]
    moved = [edges(v2, bounds[p] * PACKET, bounds[p + 1] * PACKET, 1 + p) for p in range(len(phases))]
    landed = set()

    def begin_phase(p):
        _, least, reach = phases[p]
        for hop in range(reach):
            if hop not in landed:
                land(hop)
                landed.add(hop)
        gather(bounds[p], bounds[p + 1], range(least, reach + 1))
        for copy in moved[p]:
            copy.start()

    def end_phase(p):
        for copy in moved[p]:
            copy.wait_recv()
        combine(bounds[p], bounds[p + 1])

    if len(phases) < 3:
        for hop in range(1, HALF):
            for c in range(hops[hop]):
                forward(hop, c)
        for copy in edges1:
            copy.wait_recv()
        near_groups(0, groups)
        for p in range(len(phases)):
            begin_phase(p)
            end_phase(p)
    else:
        early = [(hop, c) for hop in (1, 2) for c in range(hops[hop])]
        share = -(-groups // (len(early) - 1))
        done = began = 0
        for i, (hop, c) in enumerate(early):
            forward(hop, c)
            if i == 0:
                for copy in edges1:
                    copy.wait_recv()
            upto = min(groups, done + share)
            if upto > done:
                near_groups(done, upto)
            done = upto
            if phases[0][2] == 1 and i == hops[1] - 1:
                begin_phase(0)
                began = 1
        if began:
            end_phase(0)
        begin_phase(began)
        for c in range(hops[3]):
            forward(3, c)
        end_phase(began)
        for p in range(began + 1, len(phases)):
            begin_phase(p)
            if p > began + 1:
                end_phase(p - 1)
        end_phase(len(phases) - 1)

    for copy in edges1:
        copy.wait_send()
    for pair in moved:
        for copy in pair:
            copy.wait_send()
    for way in range(2):
        for hop in range(HALF):
            for c in range(hops[hop]):
                arrival(way, hop, c).wait_send()


def exchange(index, tab, ratios, potentials):
    plan = PLANS[index]
    hops, phases = plan
    rows, columns = potentials.shape[1:]
    blocks = columns // LANES
    _, number = chunk_base(hops)
    packets = blocks // GROUP * PACKET
    tall = rows + 2 * EDGE
    f32 = jnp.float32
    smem = pl.BlockSpec(memory_space=pltpu.SMEM)
    return pl.pallas_call(
        functools.partial(exchange_kernel, plan),
        out_shape=jax.ShapeDtypeStruct((blocks, 6 * rows, LANES), f32),
        in_specs=[smem, smem, pl.BlockSpec(memory_space=pl.ANY)],
        out_specs=pl.BlockSpec(memory_space=pltpu.VMEM),
        scratch_shapes=[
            pltpu.VMEM((rows, columns), f32),
            pltpu.VMEM((rows, columns), f32),
            pltpu.VMEM((blocks, rows, LANES), f32),
            pltpu.VMEM((2 * hops[0] * PACKET, rows, LANES), f32),
            *[pltpu.VMEM((2 * store_size(hops, i) * PACKET, rows, LANES), f32) for i in range(len(STORES))],
            pltpu.VMEM((blocks, tall, LANES), f32),
            pltpu.VMEM((packets, tall, LANES), f32),
            pltpu.VMEM((blocks, 5 * rows, LANES), f32),
            pltpu.VMEM((GROUP, tall, LANES), f32),
            pltpu.SemaphoreType.DMA((2,)),
            pltpu.SemaphoreType.DMA((2 * number,)),
            pltpu.SemaphoreType.DMA((2 * number,)),
            pltpu.SemaphoreType.DMA((2 + 2 * len(phases),)),
            pltpu.SemaphoreType.DMA((2 + 2 * len(phases),)),
        ],
        compiler_params=pltpu.CompilerParams(
            collective_id=index, has_side_effects=True, vmem_limit_bytes=30 * 2**20
        ),
        name=f"exchange{index}",
    )(tab, ratios, potentials)


def arrange_kernel(tab, fields, conv, shear, rot, disp):
    g = pl.program_id(0)
    rows, wide = conv.shape
    for j in range(wide // LANES):
        value = fields[tab[8, g * (wide // LANES) + j]]
        part = [value[k * rows : (k + 1) * rows] for k in range(6)]
        spot = slice(j * LANES, (j + 1) * LANES)
        conv[:, spot] = part[0]
        shear[0, :, spot] = part[1]
        shear[1, :, spot] = part[2]
        rot[:, spot] = part[3]
        disp[0, :, spot] = part[4]
        disp[1, :, spot] = part[5]


def arrange(tab, fields, rows):
    columns = fields.shape[0] * LANES
    wide = columns // 4
    f32 = jnp.float32
    flat = jax.ShapeDtypeStruct((rows, columns), f32)
    pair = jax.ShapeDtypeStruct((2, rows, columns), f32)
    flat_spec = pl.BlockSpec((rows, wide), lambda g: (0, g))
    pair_spec = pl.BlockSpec((2, rows, wide), lambda g: (0, 0, g))
    return pl.pallas_call(
        arrange_kernel,
        grid=(columns // wide,),
        out_shape=(flat, pair, flat, pair),
        in_specs=[pl.BlockSpec(memory_space=pltpu.SMEM), pl.BlockSpec(memory_space=pltpu.VMEM)],
        out_specs=(flat_spec, pair_spec, flat_spec, pair_spec),
        compiler_params=pltpu.CompilerParams(vmem_limit_bytes=16 * 2**20),
        name="arrange",
    )(tab, fields)


def per_device(potentials, ratios, row_offset, col_offset):
    blocks = row_offset.shape[0]
    vmem = pl.BlockSpec(memory_space=pltpu.VMEM)
    tab = pl.pallas_call(
        table_kernel,
        out_shape=jax.ShapeDtypeStruct((16, blocks), jnp.int32),
        in_specs=[vmem, vmem],
        out_specs=vmem,
        name="table",
    )(row_offset.reshape(1, blocks), col_offset.reshape(1, blocks))
    def run(index, tab, ratios, potentials):
        return arrange(tab, exchange(index, tab, ratios, potentials), potentials.shape[1])

    return lax.switch(
        tab[9, 0], [functools.partial(run, i) for i in range(len(PLANS))], tab, ratios, potentials
    )


def solution(mesh):
    return jax.shard_map(
        per_device,
        mesh=mesh,
        in_specs=(P("cosmo", "row", None), P("cosmo"), P("cosmo"), P("cosmo")),
        out_specs=(
            P(("cosmo", "row"), None),
            P(None, ("cosmo", "row"), None),
            P(("cosmo", "row"), None),
            P(None, ("cosmo", "row"), None),
        ),
        check_vma=False,
    )
```

```python
import functools

import jax
import jax.numpy as jnp
from jax import lax
from jax.experimental import pallas as pl
from jax.experimental.pallas import tpu as pltpu
from jax.sharding import PartitionSpec as P

RB = 8
LANES = 128
HALF = RB // 2
GROUP = 16
PACKET = GROUP + 1
EDGE = 4
MESH = pl.DeviceIdType.MESH

PLANS = (
    ((4, 3, 2, 1), ((2, 0, 1), (4, 1, 2), (6, 2, 3), (8, 3, 4))),
    ((5, 4, 3, 2), ((3, 0, 2), (6, 1, 3), (8, 2, 4))),
    ((8, 8, 8, 4), ((8, 0, 4),)),
)
STORES = ((0,), (1,), (2,), (3,))


def chunk_base(hops):
    base, total = [], 0
    for count in hops:
        base.append(total)
        total += count
    return base, total


def store_of(hop):
    return [i for i, members in enumerate(STORES) if hop in members][0]


def store_size(hops, i):
    return sum(hops[hop] for hop in STORES[i])


def store_base(hops, hop):
    members = STORES[store_of(hop)]
    return sum(hops[other] for other in members if other < hop)


def iota(shape, dim):
    return lax.broadcasted_iota(jnp.int32, shape, dim)


def table_kernel(row_ref, col_ref, tab_ref):
    blocks = row_ref.shape[1]
    square = (blocks, blocks)
    f32 = jnp.float32
    row = row_ref[...].astype(f32)
    lane_f = iota((1, blocks), 1).astype(f32)
    source = lane_f + col_ref[...].astype(f32)
    source = jnp.where(source >= blocks, source - blocks, source)
    sub2 = iota(square, 0)
    lane2 = iota(square, 1)
    lane2_f = lane2.astype(f32)

    def spread(v):
        return jnp.broadcast_to(v, square)

    def column(v):
        return spread(jnp.sum(jnp.where(sub2 == lane2, spread(v), 0.0), axis=1, keepdims=True))

    def total(v):
        return jnp.sum(v, axis=1, keepdims=True)

    def down(v):
        return jnp.sum(v, axis=0, keepdims=True)

    halfway = (row == HALF).astype(f32)
    dist = jnp.where(row <= HALF, row, RB - row)
    n_half = total(halfway)
    load_a = total(jnp.where(row < HALF, row, 0.0))
    load_b = total(jnp.where(row > HALF, RB - row, 0.0))
    take_a = jnp.clip(jnp.floor((load_b + HALF * n_half - load_a) / (2 * HALF) + 0.5), 0.0, n_half)

    def room(side):
        most = n_half
        for hop, count in enumerate(PLANS[0][0]):
            most = jnp.minimum(most, count * GROUP - total((side & (dist > hop)).astype(f32)))
        return most

    room_a, room_b = room((row > 0) & (row < HALF)), room(row > HALF)
    held = jnp.minimum(jnp.maximum(take_a, n_half - room_b), room_a)
    possible = (room_a >= 0) & (room_b >= 0) & (room_a + room_b >= n_half)
    take_a = jnp.where(possible, held, take_a)
    rank_half = down(jnp.where(sub2 < lane2, column(halfway), 0.0))
    way = jnp.where(row == 0, 0.0, jnp.where(row < HALF, 1.0, 2.0))
    way = jnp.where((row == HALF) & (rank_half < take_a), 1.0, way)
    big = 4096.0
    key = way * big + (HALF - dist) * blocks + lane_f
    key_c = column(key)
    slot = down(((key_c < spread(key)) & (key_c >= spread(way * big))).astype(f32))
    near = dist * blocks + lane_f
    near_c = column(near)
    place = down((near_c < spread(near)).astype(f32))

    def fitting(plan):
        hops, phases = plan
        fits = jnp.ones((1, 1), f32)
        for hop, count in enumerate(hops):
            for w in (1.0, 2.0):
                fits = jnp.where(total(((way == w) & (dist > hop)).astype(f32)) > count * GROUP, 0.0, fits)
        start = 0
        for end, least, reach in phases:
            fits = jnp.where(total((dist < least).astype(f32)) > start * GROUP, 0.0, fits)
            fits = jnp.where(total((dist <= reach).astype(f32)) < end * GROUP, 0.0, fits)
            start = end
        return fits

    fits = [fitting(plan) for plan in PLANS[:-1]]
    choice = jnp.full((1, 1), float(len(PLANS) - 1), f32)
    for i in reversed(range(len(PLANS) - 1)):
        choice = jnp.where(fits[i] > 0, float(i), choice)

    chunk = jnp.floor(slot / GROUP)
    within = slot - chunk * GROUP
    spot = []
    for hops, _ in PLANS:
        at = jnp.zeros((1, blocks), f32)
        for hop in range(HALF):
            other = jnp.where(way == 2.0, float(store_size(hops, store_of(hop))), 0.0)
            at = jnp.where(dist == hop + 1, other + float(store_base(hops, hop)), at)
        spot.append(at + chunk)
    spot = functools.reduce(lambda rest, i: jnp.where(choice == i, spot[i], rest), range(len(PLANS) - 1), spot[-1])
    spot = jnp.where(way == 0, 0.0, spot)
    within = jnp.where(way == 0, 0.0, within)
    slot_c, way_c, source_c, place_c = column(slot), column(way), column(source), column(place)
    here = slot_c == lane2_f
    send = [down(jnp.where(here & (way_c == w), source_c, 0.0)) for w in (1.0, 2.0)]
    there = place_c == lane2_f

    def ordered(v):
        return down(jnp.where(there, column(v), 0.0))

    at = ordered(spot)
    inside = ordered(within)
    kind = ordered(dist)
    turn = 8.0 * (lane_f - GROUP * jnp.floor(lane_f / GROUP) - inside) + jnp.where(kind == 0, 4.0, 0.0)
    turn = jnp.where(turn < 0, turn + LANES, turn)
    rows = [
        send[0],
        send[1],
        at * PACKET + inside,
        at * PACKET + GROUP,
        turn,
        down(jnp.where(there, source_c, 0.0)),
        kind,
        down(jnp.where(there, sub2.astype(f32), 0.0)),
        place,
        spread(choice)[:1],
    ]
    rows += [jnp.zeros((1, blocks), f32)] * (16 - len(rows))
    tab_ref[...] = jnp.concatenate(rows, axis=0).astype(jnp.int32)


def exchange_kernel(plan, tab, ratios, pot, out, p1, p2, tiles, sent, got_a, got_b, got_c, got_d, v1, v2, near, c1s,
                    local_sem, send_sem, recv_sem, edge_send, edge_recv):
    hops, phases = plan
    base, number = chunk_base(hops)
    stores = (got_a, got_b, got_c, got_d)
    size = lax.axis_size("row")
    stride = size // RB
    me = lax.axis_index("row")
    blocks = tiles.shape[0]
    rows = tiles.shape[1]
    tall = rows + 2 * EDGE
    first = hops[0]

    load2 = pltpu.make_async_copy(pot.at[1], p2, local_sem.at[0])
    load1 = pltpu.make_async_copy(pot.at[0], p1, local_sem.at[1])
    load2.start()
    load1.start()
    barrier = pltpu.get_barrier_semaphore()
    for by in (stride, size - stride, 1, size - 1):
        pl.semaphore_signal(barrier, inc=1, device_id={"row": lax.rem(me + by, size)}, device_id_type=MESH)

    lane = iota((rows, LANES), 1)
    lane_group = lane // 8

    def split(source, put):
        def body(i, carry):
            for j in range(GROUP):
                b = i * GROUP + j
                put(b, source[:, pl.ds(pl.multiple_of(b * LANES, LANES), LANES)])
            return carry

        lax.fori_loop(0, blocks // GROUP, body, 0)

    def put_tile(b, value):
        tiles[b] = value

    def put_v1(b, value):
        v1[b, EDGE : EDGE + rows, :] = value

    def sides(s):
        before = tiles[(s + (blocks - 1)) & (blocks - 1)]
        after = tiles[(s + 1) & (blocks - 1)]
        return jnp.where(lane >= LANES // 2, before, after)

    def pack(i):
        way = lax.rem(i, 2)
        chunk = i // 2
        halo = jnp.zeros((rows, LANES), jnp.float32)
        for j in range(GROUP):
            s = tab[way, chunk * GROUP + j]
            sent[i * PACKET + j] = tiles[s]
            halo = jnp.where(lane_group == j, pltpu.roll(sides(s), (8 * j + 4) % LANES, 1), halo)
        sent[i * PACKET + GROUP] = halo

    def first_copy(i):
        way = lax.rem(i, 2)
        to = way * number + i // 2
        land = way * store_size(hops, 0) + i // 2
        return pltpu.make_async_remote_copy(
            src_ref=sent.at[pl.ds(i * PACKET, PACKET)],
            dst_ref=got_a.at[pl.ds(land * PACKET, PACKET)],
            send_sem=send_sem.at[to],
            recv_sem=recv_sem.at[to],
            device_id={"row": lax.rem(me + jnp.where(way == 0, size - stride, stride), size)},
            device_id_type=MESH,
        )

    def piece(way, hop, c):
        where = store_of(hop)
        at = way * store_size(hops, where) + store_base(hops, hop) + c
        return stores[where].at[pl.ds(at * PACKET, PACKET)]

    def relay(way, hop, c):
        to = way * number + base[hop] + c
        return pltpu.make_async_remote_copy(
            src_ref=piece(way, hop - 1, c),
            dst_ref=piece(way, hop, c),
            send_sem=send_sem.at[to],
            recv_sem=recv_sem.at[to],
            device_id={"row": lax.rem(me + (size - stride if way == 0 else stride), size)},
            device_id_type=MESH,
        )

    def arrival(way, hop, c):
        to = way * number + base[hop] + c
        here = piece(way, hop, c)
        return pltpu.make_async_remote_copy(
            src_ref=here, dst_ref=here, send_sem=send_sem.at[to], recv_sem=recv_sem.at[to],
            device_id={"row": lax.rem(me + stride, size)}, device_id_type=MESH,
        )

    def edges(ref, begin, end, at):
        span = pl.ds(begin, end - begin)
        pair = []
        for k, (src, dst, by) in enumerate(((rows, 0, 1), (EDGE, EDGE + rows, size - 1))):
            pair.append(
                pltpu.make_async_remote_copy(
                    src_ref=ref.at[span, src : src + EDGE, :],
                    dst_ref=ref.at[span, dst : dst + EDGE, :],
                    send_sem=edge_send.at[2 * at + k],
                    recv_sem=edge_recv.at[2 * at + k],
                    device_id={"row": lax.rem(me + by, size)},
                    device_id_type=MESH,
                )
            )
        return pair

    load2.wait()
    split(p2, put_tile)
    pack(0)
    pl.semaphore_wait(barrier, 4)

    def step(i, carry):
        pack(i)
        first_copy(i - 1).start()
        return carry

    lax.fori_loop(1, 2 * first, step, 0)
    first_copy(2 * first - 1).start()

    load1.wait()
    split(p1, put_v1)
    edges1 = edges(v1, 0, blocks, 0)
    for copy in edges1:
        copy.start()

    near_far, beta_one, beta_two = ratios[0], ratios[1], ratios[2]
    one = 1.0 / 12.0
    two = 1.0 / 144.0

    def second(x, s1, s2, s3, s4):
        return 16.0 * (s1 - s3) + 64.0 * s2 + s4 - 130.0 * x

    sub = iota((8, LANES), 0)
    lane8 = iota((8, LANES), 1)
    eight = rows // 2

    def thirds(ref, f):
        even = ref[f, pl.ds(EDGE, eight, stride=2), :]
        odd = ref[f, pl.ds(EDGE + 1, eight, stride=2), :]
        return even, odd, jnp.where(sub < EDGE, ref[f, 0:8, :], ref[f, tall - 8 : tall, :])

    def derive(ref, f, t, j):
        x = thirds(ref, f)

        def ahead(p, k):
            return pltpu.roll(jnp.where(lane8 < k, t[p], x[p]), LANES - k, 1)

        def behind(p, k):
            return pltpu.roll(jnp.where(lane8 >= LANES - k, t[p], x[p]), k, 1)

        slope_c, curve_cc = [], []
        for p in range(3):
            a1, b1, a2, b2 = ahead(p, 1), behind(p, 1), ahead(p, 2), behind(p, 2)
            slope_c.append(8.0 * (a1 - b1) - (a2 - b2))
            if p < 2:
                curve_cc.append(second(x[p], a1 + b1, a2 + b2, ahead(p, 3) + behind(p, 3), ahead(p, 4) + behind(p, 4)))
        for p in range(2):
            c1s[j, pl.ds(EDGE + p, eight, stride=2), :] = slope_c[p]
        c1s[j, 0:EDGE, :] = slope_c[2][:EDGE]
        c1s[j, tall - EDGE : tall, :] = slope_c[2][EDGE:]
        c = {EDGE: slope_c[0], EDGE + 1: slope_c[1]}
        r = {EDGE: x[0], EDGE + 1: x[1]}
        for at in (2, 3, 6, 7):
            c[at] = c1s[j, pl.ds(at, eight, stride=2), :]
        for at in (0, 1, 2, 3, 6, 7, 8, 9):
            r[at] = ref[f, pl.ds(at, eight, stride=2), :]
        slope_r, curve_rr, curve_rc = [], [], []
        for p in range(2):
            m = EDGE + p
            slope_r.append(8.0 * (r[m + 1] - r[m - 1]) - (r[m + 2] - r[m - 2]))
            curve_rr.append(second(r[m], *[r[m + k] + r[m - k] for k in range(1, 5)]))
            curve_rc.append(8.0 * (c[m + 1] - c[m - 1]) - (c[m + 2] - c[m - 2]))
        return slope_r, slope_c, curve_rr, curve_rc, curve_cc

    def near_group(g):
        for j in range(GROUP):
            b = g * GROUP + j
            before = thirds(v1, b - 1 if j > 0 else lax.rem(b + (blocks - 1), blocks))
            after = thirds(v1, b + 1 if j < GROUP - 1 else lax.rem(b + 1, blocks))
            t = [jnp.where(lane8 >= LANES // 2, before[p], after[p]) for p in range(3)]
            slope_r, slope_c, curve_rr, curve_rc, curve_cc = derive(v1, b, t, j)
            for p in range(2):
                values = (
                    two * (curve_rr[p] + curve_cc[p]),
                    two * (curve_cc[p] - curve_rr[p]),
                    (2.0 * two) * curve_rc[p],
                    (one * beta_one) * slope_r[p],
                    (one * beta_one) * slope_c[p],
                )
                for k, value in enumerate(values):
                    near[b, k * rows + p * eight : k * rows + (p + 1) * eight, :] = value

    def near_groups(begin, end):
        def body(g, carry):
            near_group(g)
            return carry

        lax.fori_loop(begin, end, body, 0)

    def gather(begin, end, kinds):
        def body(g, carry):
            halo = jnp.zeros((rows, LANES), jnp.float32)
            for j in range(GROUP):
                f = g * GROUP + j
                kind = jnp.full((rows, LANES), tab[6, f], jnp.int32)
                value = cols = None
                for k in kinds:
                    if k == 0:
                        s = tab[5, f]
                        v, c = tiles[s], sides(s)
                    else:
                        ref = stores[k - 1]
                        at_v, at_c = tab[2, f], tab[3, f]
                        if any(k2 > 0 and stores[k2 - 1].shape[0] > ref.shape[0] for k2 in kinds):
                            at_v, at_c = jnp.minimum(at_v, ref.shape[0] - 1), jnp.minimum(at_c, ref.shape[0] - 1)
                        v, c = ref[at_v], ref[at_c]
                    value = v if value is None else jnp.where(kind == k, v, value)
                    cols = c if cols is None else jnp.where(kind == k, c, cols)
                halo = jnp.where(lane_group == j, pltpu.roll(cols, tab[4, f], 1), halo)
                v2[g * PACKET + j, EDGE : EDGE + rows, :] = value
            v2[g * PACKET + GROUP, EDGE : EDGE + rows, :] = halo
            return carry

        lax.fori_loop(begin, end, body, 0)

    scale = 0.5 * two * beta_two
    half_far = 0.5 * near_far
    half_one = 0.5 * beta_one
    slope_scale = one * beta_two

    def combine(begin, end):
        def body(g, carry):
            halo = thirds(v2, g * PACKET + GROUP)
            for j in range(GROUP):
                f = g * GROUP + j
                t = [pltpu.roll(h, (LANES - 8 * j - 4) % LANES, 1) for h in halo]
                far_r, far_c, far_rr, far_rc, far_cc = derive(v2, g * PACKET + j, t, j)
                n = near[tab[7, f]]
                for p in range(2):
                    n_sum, n_diff, n_rc2, n_r, n_c = (
                        n[k * rows + p * eight : k * rows + (p + 1) * eight] for k in range(5)
                    )
                    s = scale * (far_rr[p] + far_cc[p])
                    d = scale * (far_cc[p] - far_rr[p])
                    r = scale * far_rc[p]
                    d_half = half_far * d
                    r_far = near_far * r
                    rest = half_one - half_far * s
                    results = (
                        s + n_sum * rest - d_half * n_diff - r_far * n_rc2,
                        d + n_diff * rest - d_half * n_sum,
                        (r + r) + n_rc2 * rest - r_far * n_sum,
                        r_far * n_diff - n_rc2 * d_half,
                        n_r + slope_scale * far_r[p],
                        n_c + slope_scale * far_c[p],
                    )
                    for k, value in enumerate(results):
                        out[f, pl.ds(k * rows + p, eight, stride=2), :] = value
            return carry

        lax.fori_loop(begin, end, body, 0)

    def forward(hop, c):
        for way in range(2):
            arrival(way, hop - 1, c).wait_recv()
            relay(way, hop, c).start()

    def land(hop):
        for c in range(hops[hop + 1] if hop + 1 < HALF else 0, hops[hop]):
            for way in range(2):
                arrival(way, hop, c).wait_recv()

    groups = blocks // GROUP
    bounds = [0] + [end for end, _, _ in phases]
    moved = [edges(v2, bounds[p] * PACKET, bounds[p + 1] * PACKET, 1 + p) for p in range(len(phases))]
    landed = set()

    def begin_phase(p):
        _, least, reach = phases[p]
        for hop in range(reach):
            if hop not in landed:
                land(hop)
                landed.add(hop)
        gather(bounds[p], bounds[p + 1], range(least, reach + 1))
        for copy in moved[p]:
            copy.start()

    def end_phase(p):
        for copy in moved[p]:
            copy.wait_recv()
        combine(bounds[p], bounds[p + 1])

    if len(phases) < 3:
        for hop in range(1, HALF):
            for c in range(hops[hop]):
                forward(hop, c)
        for copy in edges1:
            copy.wait_recv()
        near_groups(0, groups)
        for p in range(len(phases)):
            begin_phase(p)
            end_phase(p)
    else:
        early = [(hop, c) for hop in (1, 2) for c in range(hops[hop])]
        share = -(-groups // (len(early) - 1))
        done = began = 0
        for i, (hop, c) in enumerate(early):
            forward(hop, c)
            if i == 0:
                for copy in edges1:
                    copy.wait_recv()
            upto = min(groups, done + share)
            if upto > done:
                near_groups(done, upto)
            done = upto
            if phases[0][2] == 1 and i == hops[1] - 1:
                begin_phase(0)
                began = 1
        if began:
            end_phase(0)
        begin_phase(began)
        for c in range(hops[3]):
            forward(3, c)
        end_phase(began)
        for p in range(began + 1, len(phases)):
            begin_phase(p)
            if p > began + 1:
                end_phase(p - 1)
        end_phase(len(phases) - 1)

    for copy in edges1:
        copy.wait_send()
    for pair in moved:
        for copy in pair:
            copy.wait_send()
    for way in range(2):
        for hop in range(HALF):
            for c in range(hops[hop]):
                arrival(way, hop, c).wait_send()


def exchange(index, tab, ratios, potentials):
    plan = PLANS[index]
    hops, phases = plan
    rows, columns = potentials.shape[1:]
    blocks = columns // LANES
    _, number = chunk_base(hops)
    packets = blocks // GROUP * PACKET
    tall = rows + 2 * EDGE
    f32 = jnp.float32
    smem = pl.BlockSpec(memory_space=pltpu.SMEM)
    return pl.pallas_call(
        functools.partial(exchange_kernel, plan),
        out_shape=jax.ShapeDtypeStruct((blocks, 6 * rows, LANES), f32),
        in_specs=[smem, smem, pl.BlockSpec(memory_space=pl.ANY)],
        out_specs=pl.BlockSpec(memory_space=pltpu.VMEM),
        scratch_shapes=[
            pltpu.VMEM((rows, columns), f32),
            pltpu.VMEM((rows, columns), f32),
            pltpu.VMEM((blocks, rows, LANES), f32),
            pltpu.VMEM((2 * hops[0] * PACKET, rows, LANES), f32),
            *[pltpu.VMEM((2 * store_size(hops, i) * PACKET, rows, LANES), f32) for i in range(len(STORES))],
            pltpu.VMEM((blocks, tall, LANES), f32),
            pltpu.VMEM((packets, tall, LANES), f32),
            pltpu.VMEM((blocks, 5 * rows, LANES), f32),
            pltpu.VMEM((GROUP, tall, LANES), f32),
            pltpu.SemaphoreType.DMA((2,)),
            pltpu.SemaphoreType.DMA((2 * number,)),
            pltpu.SemaphoreType.DMA((2 * number,)),
            pltpu.SemaphoreType.DMA((2 + 2 * len(phases),)),
            pltpu.SemaphoreType.DMA((2 + 2 * len(phases),)),
        ],
        compiler_params=pltpu.CompilerParams(
            collective_id=index, has_side_effects=True, vmem_limit_bytes=30 * 2**20
        ),
        name=f"exchange{index}",
    )(tab, ratios, potentials)


def arrange_kernel(tab, fields, conv, shear, rot, disp):
    g = pl.program_id(0)
    rows, wide = conv.shape
    for j in range(wide // LANES):
        value = fields[tab[8, g * (wide // LANES) + j]]
        part = [value[k * rows : (k + 1) * rows] for k in range(6)]
        spot = slice(j * LANES, (j + 1) * LANES)
        conv[:, spot] = part[0]
        shear[0, :, spot] = part[1]
        shear[1, :, spot] = part[2]
        rot[:, spot] = part[3]
        disp[0, :, spot] = part[4]
        disp[1, :, spot] = part[5]


def arrange(tab, fields, rows):
    columns = fields.shape[0] * LANES
    wide = columns // 4
    f32 = jnp.float32
    flat = jax.ShapeDtypeStruct((rows, columns), f32)
    pair = jax.ShapeDtypeStruct((2, rows, columns), f32)
    flat_spec = pl.BlockSpec((rows, wide), lambda g: (0, g))
    pair_spec = pl.BlockSpec((2, rows, wide), lambda g: (0, 0, g))
    return pl.pallas_call(
        arrange_kernel,
        grid=(columns // wide,),
        out_shape=(flat, pair, flat, pair),
        in_specs=[pl.BlockSpec(memory_space=pltpu.SMEM), pl.BlockSpec(memory_space=pltpu.VMEM)],
        out_specs=(flat_spec, pair_spec, flat_spec, pair_spec),
        compiler_params=pltpu.CompilerParams(vmem_limit_bytes=16 * 2**20),
        name="arrange",
    )(tab, fields)


def per_device(potentials, ratios, row_offset, col_offset):
    blocks = row_offset.shape[0]
    vmem = pl.BlockSpec(memory_space=pltpu.VMEM)
    tab = pl.pallas_call(
        table_kernel,
        out_shape=jax.ShapeDtypeStruct((16, blocks), jnp.int32),
        in_specs=[vmem, vmem],
        out_specs=vmem,
        name="table",
    )(row_offset.reshape(1, blocks), col_offset.reshape(1, blocks))
    def run(index, tab, ratios, potentials):
        return arrange(tab, exchange(index, tab, ratios, potentials), potentials.shape[1])

    return lax.switch(
        tab[9, 0], [functools.partial(run, i) for i in range(len(PLANS))], tab, ratios, potentials
    )


def solution(mesh):
    return jax.shard_map(
        per_device,
        mesh=mesh,
        in_specs=(P("cosmo", "row", None), P("cosmo"), P("cosmo"), P("cosmo")),
        out_specs=(
            P(("cosmo", "row"), None),
            P(None, ("cosmo", "row"), None),
            P(("cosmo", "row"), None),
            P(None, ("cosmo", "row"), None),
        ),
        check_vma=False,
    )
```

```python
import functools

import jax
import jax.numpy as jnp
from jax import lax
from jax.experimental import pallas as pl
from jax.experimental.pallas import tpu as pltpu
from jax.sharding import PartitionSpec as P

RB = 8
LANES = 128
HALF = RB // 2
GROUP = 16
PACKET = GROUP + 1
EDGE = 4
MESH = pl.DeviceIdType.MESH

PLANS = (
    ((4, 3, 2, 1), ((2, 0, 1), (4, 1, 2), (6, 2, 3), (8, 3, 4))),
    ((5, 4, 3, 2), ((3, 0, 2), (6, 1, 3), (8, 2, 4))),
    ((8, 8, 8, 4), ((8, 0, 4),)),
)
STORES = ((0,), (1,), (2,), (3,))


def chunk_base(hops):
    base, total = [], 0
    for count in hops:
        base.append(total)
        total += count
    return base, total


def store_of(hop):
    return [i for i, members in enumerate(STORES) if hop in members][0]


def store_size(hops, i):
    return sum(hops[hop] for hop in STORES[i])


def store_base(hops, hop):
    members = STORES[store_of(hop)]
    return sum(hops[other] for other in members if other < hop)


def iota(shape, dim):
    return lax.broadcasted_iota(jnp.int32, shape, dim)


def table_kernel(row_ref, col_ref, tab_ref):
    blocks = row_ref.shape[1]
    square = (blocks, blocks)
    f32 = jnp.float32
    row = row_ref[...].astype(f32)
    lane_f = iota((1, blocks), 1).astype(f32)
    source = lane_f + col_ref[...].astype(f32)
    source = jnp.where(source >= blocks, source - blocks, source)
    sub2 = iota(square, 0)
    lane2 = iota(square, 1)
    lane2_f = lane2.astype(f32)

    def spread(v):
        return jnp.broadcast_to(v, square)

    def column(v):
        return spread(jnp.sum(jnp.where(sub2 == lane2, spread(v), 0.0), axis=1, keepdims=True))

    def total(v):
        return jnp.sum(v, axis=1, keepdims=True)

    def down(v):
        return jnp.sum(v, axis=0, keepdims=True)

    halfway = (row == HALF).astype(f32)
    dist = jnp.where(row <= HALF, row, RB - row)
    n_half = total(halfway)
    load_a = total(jnp.where(row < HALF, row, 0.0))
    load_b = total(jnp.where(row > HALF, RB - row, 0.0))
    take_a = jnp.clip(jnp.floor((load_b + HALF * n_half - load_a) / (2 * HALF) + 0.5), 0.0, n_half)

    def room(side):
        most = n_half
        for hop, count in enumerate(PLANS[0][0]):
            most = jnp.minimum(most, count * GROUP - total((side & (dist > hop)).astype(f32)))
        return most

    room_a, room_b = room((row > 0) & (row < HALF)), room(row > HALF)
    held = jnp.minimum(jnp.maximum(take_a, n_half - room_b), room_a)
    possible = (room_a >= 0) & (room_b >= 0) & (room_a + room_b >= n_half)
    take_a = jnp.where(possible, held, take_a)
    rank_half = down(jnp.where(sub2 < lane2, column(halfway), 0.0))
    way = jnp.where(row == 0, 0.0, jnp.where(row < HALF, 1.0, 2.0))
    way = jnp.where((row == HALF) & (rank_half < take_a), 1.0, way)
    big = 4096.0
    key = way * big + (HALF - dist) * blocks + lane_f
    key_c = column(key)
    slot = down(((key_c < spread(key)) & (key_c >= spread(way * big))).astype(f32))
    near = dist * blocks + lane_f
    near_c = column(near)
    place = down((near_c < spread(near)).astype(f32))

    def fitting(plan):
        hops, phases = plan
        fits = jnp.ones((1, 1), f32)
        for hop, count in enumerate(hops):
            for w in (1.0, 2.0):
                fits = jnp.where(total(((way == w) & (dist > hop)).astype(f32)) > count * GROUP, 0.0, fits)
        start = 0
        for end, least, reach in phases:
            fits = jnp.where(total((dist < least).astype(f32)) > start * GROUP, 0.0, fits)
            fits = jnp.where(total((dist <= reach).astype(f32)) < end * GROUP, 0.0, fits)
            start = end
        return fits

    fits = [fitting(plan) for plan in PLANS[:-1]]
    choice = jnp.full((1, 1), float(len(PLANS) - 1), f32)
    for i in reversed(range(len(PLANS) - 1)):
        choice = jnp.where(fits[i] > 0, float(i), choice)

    chunk = jnp.floor(slot / GROUP)
    within = slot - chunk * GROUP
    spot = []
    for hops, _ in PLANS:
        at = jnp.zeros((1, blocks), f32)
        for hop in range(HALF):
            other = jnp.where(way == 2.0, float(store_size(hops, store_of(hop))), 0.0)
            at = jnp.where(dist == hop + 1, other + float(store_base(hops, hop)), at)
        spot.append(at + chunk)
    spot = functools.reduce(lambda rest, i: jnp.where(choice == i, spot[i], rest), range(len(PLANS) - 1), spot[-1])
    spot = jnp.where(way == 0, 0.0, spot)
    within = jnp.where(way == 0, 0.0, within)
    slot_c, way_c, source_c, place_c = column(slot), column(way), column(source), column(place)
    here = slot_c == lane2_f
    send = [down(jnp.where(here & (way_c == w), source_c, 0.0)) for w in (1.0, 2.0)]
    there = place_c == lane2_f

    def ordered(v):
        return down(jnp.where(there, column(v), 0.0))

    at = ordered(spot)
    inside = ordered(within)
    kind = ordered(dist)
    turn = 8.0 * (lane_f - GROUP * jnp.floor(lane_f / GROUP) - inside) + jnp.where(kind == 0, 4.0, 0.0)
    turn = jnp.where(turn < 0, turn + LANES, turn)
    rows = [
        send[0],
        send[1],
        at * PACKET + inside,
        at * PACKET + GROUP,
        turn,
        down(jnp.where(there, source_c, 0.0)),
        kind,
        down(jnp.where(there, sub2.astype(f32), 0.0)),
        place,
        spread(choice)[:1],
    ]
    rows += [jnp.zeros((1, blocks), f32)] * (16 - len(rows))
    tab_ref[...] = jnp.concatenate(rows, axis=0).astype(jnp.int32)


def exchange_kernel(plan, tab, ratios, pot, out, p1, p2, tiles, sent, got_a, got_b, got_c, got_d, v1, v2, near, c1s, turned,
                    local_sem, send_sem, recv_sem, edge_send, edge_recv):
    hops, phases = plan
    base, number = chunk_base(hops)
    stores = (got_a, got_b, got_c, got_d)
    size = lax.axis_size("row")
    stride = size // RB
    me = lax.axis_index("row")
    blocks = tiles.shape[0]
    rows = tiles.shape[1]
    tall = rows + 2 * EDGE
    first = hops[0]

    load2 = pltpu.make_async_copy(pot.at[1], p2, local_sem.at[0])
    load1 = pltpu.make_async_copy(pot.at[0], p1, local_sem.at[1])
    load2.start()
    load1.start()
    barrier = pltpu.get_barrier_semaphore()
    for by in (stride, size - stride, 1, size - 1):
        pl.semaphore_signal(barrier, inc=1, device_id={"row": lax.rem(me + by, size)}, device_id_type=MESH)

    lane = iota((rows, LANES), 1)
    lane_group = lane // 8

    def split(source, put):
        def body(i, carry):
            for j in range(GROUP):
                b = i * GROUP + j
                put(b, source[:, pl.ds(pl.multiple_of(b * LANES, LANES), LANES)])
            return carry

        lax.fori_loop(0, blocks // GROUP, body, 0)

    def put_tile(b, value):
        tiles[b] = value

    def put_v1(b, value):
        v1[b, EDGE : EDGE + rows, :] = value

    def sides(s):
        before = tiles[(s + (blocks - 1)) & (blocks - 1)]
        after = tiles[(s + 1) & (blocks - 1)]
        return jnp.where(lane >= LANES // 2, before, after)

    def pack(i):
        way = lax.rem(i, 2)
        chunk = i // 2
        halo = jnp.zeros((rows, LANES), jnp.float32)
        for j in range(GROUP):
            s = tab[way, chunk * GROUP + j]
            sent[i * PACKET + j] = tiles[s]
            halo = jnp.where(lane_group == j, pltpu.roll(sides(s), (8 * j + 4) % LANES, 1), halo)
        sent[i * PACKET + GROUP] = halo

    def first_copy(i):
        way = lax.rem(i, 2)
        to = way * number + i // 2
        land = way * store_size(hops, 0) + i // 2
        return pltpu.make_async_remote_copy(
            src_ref=sent.at[pl.ds(i * PACKET, PACKET)],
            dst_ref=got_a.at[pl.ds(land * PACKET, PACKET)],
            send_sem=send_sem.at[to],
            recv_sem=recv_sem.at[to],
            device_id={"row": lax.rem(me + jnp.where(way == 0, size - stride, stride), size)},
            device_id_type=MESH,
        )

    def piece(way, hop, c):
        where = store_of(hop)
        at = way * store_size(hops, where) + store_base(hops, hop) + c
        return stores[where].at[pl.ds(at * PACKET, PACKET)]

    def relay(way, hop, c):
        to = way * number + base[hop] + c
        return pltpu.make_async_remote_copy(
            src_ref=piece(way, hop - 1, c),
            dst_ref=piece(way, hop, c),
            send_sem=send_sem.at[to],
            recv_sem=recv_sem.at[to],
            device_id={"row": lax.rem(me + (size - stride if way == 0 else stride), size)},
            device_id_type=MESH,
        )

    def arrival(way, hop, c):
        to = way * number + base[hop] + c
        here = piece(way, hop, c)
        return pltpu.make_async_remote_copy(
            src_ref=here, dst_ref=here, send_sem=send_sem.at[to], recv_sem=recv_sem.at[to],
            device_id={"row": lax.rem(me + stride, size)}, device_id_type=MESH,
        )

    def edges(ref, begin, end, at):
        span = pl.ds(begin, end - begin)
        pair = []
        for k, (src, dst, by) in enumerate(((rows, 0, 1), (EDGE, EDGE + rows, size - 1))):
            pair.append(
                pltpu.make_async_remote_copy(
                    src_ref=ref.at[span, src : src + EDGE, :],
                    dst_ref=ref.at[span, dst : dst + EDGE, :],
                    send_sem=edge_send.at[2 * at + k],
                    recv_sem=edge_recv.at[2 * at + k],
                    device_id={"row": lax.rem(me + by, size)},
                    device_id_type=MESH,
                )
            )
        return pair

    load2.wait()
    split(p2, put_tile)
    pack(0)
    pl.semaphore_wait(barrier, 4)

    def step(i, carry):
        pack(i)
        first_copy(i - 1).start()
        return carry

    lax.fori_loop(1, 2 * first, step, 0)
    first_copy(2 * first - 1).start()

    load1.wait()
    split(p1, put_v1)
    edges1 = edges(v1, 0, blocks, 0)
    for copy in edges1:
        copy.start()

    near_far, beta_one, beta_two = ratios[0], ratios[1], ratios[2]
    one = 1.0 / 12.0
    two = 1.0 / 144.0

    def second(x, s1, s2, s3, s4):
        return 16.0 * (s1 - s3) + 64.0 * s2 + s4 - 130.0 * x

    sub = iota((8, LANES), 0)
    lane8 = iota((8, LANES), 1)
    eight = rows // 2

    def thirds(ref, f):
        even = ref[f, pl.ds(EDGE, eight, stride=2), :]
        odd = ref[f, pl.ds(EDGE + 1, eight, stride=2), :]
        return even, odd, jnp.where(sub < EDGE, ref[f, 0:8, :], ref[f, tall - 8 : tall, :])

    def derive(ref, f, t, j):
        x = thirds(ref, f)

        def ahead(p, k):
            return pltpu.roll(jnp.where(lane8 < k, t[p], x[p]), LANES - k, 1)

        def behind(p, k):
            return pltpu.roll(jnp.where(lane8 >= LANES - k, t[p], x[p]), k, 1)

        slope_c, curve_cc = [], []
        for p in range(3):
            a1, b1, a2, b2 = ahead(p, 1), behind(p, 1), ahead(p, 2), behind(p, 2)
            slope_c.append(8.0 * (a1 - b1) - (a2 - b2))
            if p < 2:
                curve_cc.append(second(x[p], a1 + b1, a2 + b2, ahead(p, 3) + behind(p, 3), ahead(p, 4) + behind(p, 4)))
        for p in range(2):
            c1s[j, pl.ds(EDGE + p, eight, stride=2), :] = slope_c[p]
        c1s[j, 0:EDGE, :] = slope_c[2][:EDGE]
        c1s[j, tall - EDGE : tall, :] = slope_c[2][EDGE:]
        c = {EDGE: slope_c[0], EDGE + 1: slope_c[1]}
        r = {EDGE: x[0], EDGE + 1: x[1]}
        for at in (2, 3, 6, 7):
            c[at] = c1s[j, pl.ds(at, eight, stride=2), :]
        for at in (0, 1, 2, 3, 6, 7, 8, 9):
            r[at] = ref[f, pl.ds(at, eight, stride=2), :]
        slope_r, curve_rr, curve_rc = [], [], []
        for p in range(2):
            m = EDGE + p
            slope_r.append(8.0 * (r[m + 1] - r[m - 1]) - (r[m + 2] - r[m - 2]))
            curve_rr.append(second(r[m], *[r[m + k] + r[m - k] for k in range(1, 5)]))
            curve_rc.append(8.0 * (c[m + 1] - c[m - 1]) - (c[m + 2] - c[m - 2]))
        return slope_r, slope_c, curve_rr, curve_rc, curve_cc

    def near_group(g):
        for j in range(GROUP):
            b = g * GROUP + j
            before = thirds(v1, b - 1 if j > 0 else lax.rem(b + (blocks - 1), blocks))
            after = thirds(v1, b + 1 if j < GROUP - 1 else lax.rem(b + 1, blocks))
            t = [jnp.where(lane8 >= LANES // 2, before[p], after[p]) for p in range(3)]
            slope_r, slope_c, curve_rr, curve_rc, curve_cc = derive(v1, b, t, j)
            for p in range(2):
                values = (
                    two * (curve_rr[p] + curve_cc[p]),
                    two * (curve_cc[p] - curve_rr[p]),
                    (2.0 * two) * curve_rc[p],
                    (one * beta_one) * slope_r[p],
                    (one * beta_one) * slope_c[p],
                )
                for k, value in enumerate(values):
                    near[b, k * rows + p * eight : k * rows + (p + 1) * eight, :] = value

    def near_groups(begin, end):
        def body(g, carry):
            near_group(g)
            return carry

        lax.fori_loop(begin, end, body, 0)

    def gather(begin, end, kinds):
        def body(g, carry):
            halo = jnp.zeros((rows, LANES), jnp.float32)
            for j in range(GROUP):
                f = g * GROUP + j
                kind = jnp.full((rows, LANES), tab[6, f], jnp.int32)
                value = cols = None
                for k in kinds:
                    if k == 0:
                        s = tab[5, f]
                        v, c = tiles[s], sides(s)
                    else:
                        ref = stores[k - 1]
                        at_v, at_c = tab[2, f], tab[3, f]
                        if any(k2 > 0 and stores[k2 - 1].shape[0] > ref.shape[0] for k2 in kinds):
                            at_v, at_c = jnp.minimum(at_v, ref.shape[0] - 1), jnp.minimum(at_c, ref.shape[0] - 1)
                        v, c = ref[at_v], ref[at_c]
                    value = v if value is None else jnp.where(kind == k, v, value)
                    cols = c if cols is None else jnp.where(kind == k, c, cols)
                halo = jnp.where(lane_group == j, pltpu.roll(cols, tab[4, f], 1), halo)
                v2[g * PACKET + j, EDGE : EDGE + rows, :] = value
            v2[g * PACKET + GROUP, EDGE : EDGE + rows, :] = halo
            return carry

        lax.fori_loop(begin, end, body, 0)

    scale = 0.5 * two * beta_two
    half_far = 0.5 * near_far
    half_one = 0.5 * beta_one
    slope_scale = one * beta_two

    def combine(begin, end):
        def body(g, carry):
            halo = thirds(v2, g * PACKET + GROUP)
            for j in range(GROUP):
                for p in range(3):
                    turned[j, 8 * p : 8 * p + 8, :] = pltpu.roll(halo[p], (LANES - 8 * j - 4) % LANES, 1)
            for j in range(GROUP):
                f = g * GROUP + j
                t = [turned[j, 8 * p : 8 * p + 8, :] for p in range(3)]
                far_r, far_c, far_rr, far_rc, far_cc = derive(v2, g * PACKET + j, t, j)
                n = near[tab[7, f]]
                for p in range(2):
                    n_sum, n_diff, n_rc2, n_r, n_c = (
                        n[k * rows + p * eight : k * rows + (p + 1) * eight] for k in range(5)
                    )
                    s = scale * (far_rr[p] + far_cc[p])
                    d = scale * (far_cc[p] - far_rr[p])
                    r = scale * far_rc[p]
                    d_half = half_far * d
                    r_far = near_far * r
                    rest = half_one - half_far * s
                    results = (
                        s + n_sum * rest - d_half * n_diff - r_far * n_rc2,
                        d + n_diff * rest - d_half * n_sum,
                        (r + r) + n_rc2 * rest - r_far * n_sum,
                        r_far * n_diff - n_rc2 * d_half,
                        n_r + slope_scale * far_r[p],
                        n_c + slope_scale * far_c[p],
                    )
                    for k, value in enumerate(results):
                        out[f, pl.ds(k * rows + p, eight, stride=2), :] = value
            return carry

        lax.fori_loop(begin, end, body, 0)

    def forward(hop, c):
        for way in range(2):
            arrival(way, hop - 1, c).wait_recv()
            relay(way, hop, c).start()

    def land(hop):
        for c in range(hops[hop + 1] if hop + 1 < HALF else 0, hops[hop]):
            for way in range(2):
                arrival(way, hop, c).wait_recv()

    groups = blocks // GROUP
    bounds = [0] + [end for end, _, _ in phases]
    moved = [edges(v2, bounds[p] * PACKET, bounds[p + 1] * PACKET, 1 + p) for p in range(len(phases))]
    landed = set()

    def begin_phase(p):
        _, least, reach = phases[p]
        for hop in range(reach):
            if hop not in landed:
                land(hop)
                landed.add(hop)
        gather(bounds[p], bounds[p + 1], range(least, reach + 1))
        for copy in moved[p]:
            copy.start()

    def end_phase(p):
        for copy in moved[p]:
            copy.wait_recv()
        combine(bounds[p], bounds[p + 1])

    if len(phases) < 3:
        for hop in range(1, HALF):
            for c in range(hops[hop]):
                forward(hop, c)
        for copy in edges1:
            copy.wait_recv()
        near_groups(0, groups)
        for p in range(len(phases)):
            begin_phase(p)
            end_phase(p)
    else:
        early = [(hop, c) for hop in (1, 2) for c in range(hops[hop])]
        share = -(-groups // (len(early) - 1))
        done = began = 0
        for i, (hop, c) in enumerate(early):
            forward(hop, c)
            if i == 0:
                for copy in edges1:
                    copy.wait_recv()
            upto = min(groups, done + share)
            if upto > done:
                near_groups(done, upto)
            done = upto
            if phases[0][2] == 1 and i == hops[1] - 1:
                begin_phase(0)
                began = 1
        if began:
            end_phase(0)
        begin_phase(began)
        for c in range(hops[3]):
            forward(3, c)
        end_phase(began)
        for p in range(began + 1, len(phases)):
            begin_phase(p)
            if p > began + 1:
                end_phase(p - 1)
        end_phase(len(phases) - 1)

    for copy in edges1:
        copy.wait_send()
    for pair in moved:
        for copy in pair:
            copy.wait_send()
    for way in range(2):
        for hop in range(HALF):
            for c in range(hops[hop]):
                arrival(way, hop, c).wait_send()


def exchange(index, tab, ratios, potentials):
    plan = PLANS[index]
    hops, phases = plan
    rows, columns = potentials.shape[1:]
    blocks = columns // LANES
    _, number = chunk_base(hops)
    packets = blocks // GROUP * PACKET
    tall = rows + 2 * EDGE
    f32 = jnp.float32
    smem = pl.BlockSpec(memory_space=pltpu.SMEM)
    return pl.pallas_call(
        functools.partial(exchange_kernel, plan),
        out_shape=jax.ShapeDtypeStruct((blocks, 6 * rows, LANES), f32),
        in_specs=[smem, smem, pl.BlockSpec(memory_space=pl.ANY)],
        out_specs=pl.BlockSpec(memory_space=pltpu.VMEM),
        scratch_shapes=[
            pltpu.VMEM((rows, columns), f32),
            pltpu.VMEM((rows, columns), f32),
            pltpu.VMEM((blocks, rows, LANES), f32),
            pltpu.VMEM((2 * hops[0] * PACKET, rows, LANES), f32),
            *[pltpu.VMEM((2 * store_size(hops, i) * PACKET, rows, LANES), f32) for i in range(len(STORES))],
            pltpu.VMEM((blocks, tall, LANES), f32),
            pltpu.VMEM((packets, tall, LANES), f32),
            pltpu.VMEM((blocks, 5 * rows, LANES), f32),
            pltpu.VMEM((GROUP, tall, LANES), f32),
            pltpu.VMEM((GROUP, tall, LANES), f32),
            pltpu.SemaphoreType.DMA((2,)),
            pltpu.SemaphoreType.DMA((2 * number,)),
            pltpu.SemaphoreType.DMA((2 * number,)),
            pltpu.SemaphoreType.DMA((2 + 2 * len(phases),)),
            pltpu.SemaphoreType.DMA((2 + 2 * len(phases),)),
        ],
        compiler_params=pltpu.CompilerParams(
            collective_id=index, has_side_effects=True, vmem_limit_bytes=30 * 2**20
        ),
        name=f"exchange{index}",
    )(tab, ratios, potentials)


def arrange_kernel(tab, fields, conv, shear, rot, disp):
    g = pl.program_id(0)
    rows, wide = conv.shape
    for j in range(wide // LANES):
        value = fields[tab[8, g * (wide // LANES) + j]]
        part = [value[k * rows : (k + 1) * rows] for k in range(6)]
        spot = slice(j * LANES, (j + 1) * LANES)
        conv[:, spot] = part[0]
        shear[0, :, spot] = part[1]
        shear[1, :, spot] = part[2]
        rot[:, spot] = part[3]
        disp[0, :, spot] = part[4]
        disp[1, :, spot] = part[5]


def arrange(tab, fields, rows):
    columns = fields.shape[0] * LANES
    wide = columns // 4
    f32 = jnp.float32
    flat = jax.ShapeDtypeStruct((rows, columns), f32)
    pair = jax.ShapeDtypeStruct((2, rows, columns), f32)
    flat_spec = pl.BlockSpec((rows, wide), lambda g: (0, g))
    pair_spec = pl.BlockSpec((2, rows, wide), lambda g: (0, 0, g))
    return pl.pallas_call(
        arrange_kernel,
        grid=(columns // wide,),
        out_shape=(flat, pair, flat, pair),
        in_specs=[pl.BlockSpec(memory_space=pltpu.SMEM), pl.BlockSpec(memory_space=pltpu.VMEM)],
        out_specs=(flat_spec, pair_spec, flat_spec, pair_spec),
        compiler_params=pltpu.CompilerParams(vmem_limit_bytes=16 * 2**20),
        name="arrange",
    )(tab, fields)


def per_device(potentials, ratios, row_offset, col_offset):
    blocks = row_offset.shape[0]
    vmem = pl.BlockSpec(memory_space=pltpu.VMEM)
    tab = pl.pallas_call(
        table_kernel,
        out_shape=jax.ShapeDtypeStruct((16, blocks), jnp.int32),
        in_specs=[vmem, vmem],
        out_specs=vmem,
        name="table",
    )(row_offset.reshape(1, blocks), col_offset.reshape(1, blocks))
    def run(index, tab, ratios, potentials):
        return arrange(tab, exchange(index, tab, ratios, potentials), potentials.shape[1])

    return lax.switch(
        tab[9, 0], [functools.partial(run, i) for i in range(len(PLANS))], tab, ratios, potentials
    )


def solution(mesh):
    return jax.shard_map(
        per_device,
        mesh=mesh,
        in_specs=(P("cosmo", "row", None), P("cosmo"), P("cosmo"), P("cosmo")),
        out_specs=(
            P(("cosmo", "row"), None),
            P(None, ("cosmo", "row"), None),
            P(("cosmo", "row"), None),
            P(None, ("cosmo", "row"), None),
        ),
        check_vma=False,
    )
```

```python
import functools

import jax
import jax.numpy as jnp
from jax import lax
from jax.experimental import pallas as pl
from jax.experimental.pallas import tpu as pltpu
from jax.sharding import PartitionSpec as P

RB = 8
LANES = 128
HALF = RB // 2
GROUP = 16
PACKET = GROUP + 1
EDGE = 4
MESH = pl.DeviceIdType.MESH

PLANS = (
    ((4, 3, 2, 1), ((2, 0, 1), (4, 1, 2), (6, 2, 3), (8, 3, 4))),
    ((5, 4, 3, 2), ((3, 0, 2), (6, 1, 3), (8, 2, 4))),
    ((8, 8, 8, 4), ((8, 0, 4),)),
)
STORES = ((0,), (1,), (2,), (3,))


def chunk_base(hops):
    base, total = [], 0
    for count in hops:
        base.append(total)
        total += count
    return base, total


def store_of(hop):
    return [i for i, members in enumerate(STORES) if hop in members][0]


def store_size(hops, i):
    return sum(hops[hop] for hop in STORES[i])


def store_base(hops, hop):
    members = STORES[store_of(hop)]
    return sum(hops[other] for other in members if other < hop)


def iota(shape, dim):
    return lax.broadcasted_iota(jnp.int32, shape, dim)


def table_kernel(row_ref, col_ref, tab_ref):
    blocks = row_ref.shape[1]
    square = (blocks, blocks)
    f32 = jnp.float32
    row = row_ref[...].astype(f32)
    lane_f = iota((1, blocks), 1).astype(f32)
    source = lane_f + col_ref[...].astype(f32)
    source = jnp.where(source >= blocks, source - blocks, source)
    sub2 = iota(square, 0)
    lane2 = iota(square, 1)
    lane2_f = lane2.astype(f32)

    def spread(v):
        return jnp.broadcast_to(v, square)

    def column(v):
        return spread(jnp.sum(jnp.where(sub2 == lane2, spread(v), 0.0), axis=1, keepdims=True))

    def total(v):
        return jnp.sum(v, axis=1, keepdims=True)

    def down(v):
        return jnp.sum(v, axis=0, keepdims=True)

    halfway = (row == HALF).astype(f32)
    dist = jnp.where(row <= HALF, row, RB - row)
    n_half = total(halfway)
    load_a = total(jnp.where(row < HALF, row, 0.0))
    load_b = total(jnp.where(row > HALF, RB - row, 0.0))
    take_a = jnp.clip(jnp.floor((load_b + HALF * n_half - load_a) / (2 * HALF) + 0.5), 0.0, n_half)

    def room(side):
        most = n_half
        for hop, count in enumerate(PLANS[0][0]):
            most = jnp.minimum(most, count * GROUP - total((side & (dist > hop)).astype(f32)))
        return most

    room_a, room_b = room((row > 0) & (row < HALF)), room(row > HALF)
    held = jnp.minimum(jnp.maximum(take_a, n_half - room_b), room_a)
    possible = (room_a >= 0) & (room_b >= 0) & (room_a + room_b >= n_half)
    take_a = jnp.where(possible, held, take_a)
    rank_half = down(jnp.where(sub2 < lane2, column(halfway), 0.0))
    way = jnp.where(row == 0, 0.0, jnp.where(row < HALF, 1.0, 2.0))
    way = jnp.where((row == HALF) & (rank_half < take_a), 1.0, way)
    big = 4096.0
    key = way * big + (HALF - dist) * blocks + lane_f
    key_c = column(key)
    slot = down(((key_c < spread(key)) & (key_c >= spread(way * big))).astype(f32))
    near = dist * blocks + lane_f
    near_c = column(near)
    place = down((near_c < spread(near)).astype(f32))

    def fitting(plan):
        hops, phases = plan
        fits = jnp.ones((1, 1), f32)
        for hop, count in enumerate(hops):
            for w in (1.0, 2.0):
                fits = jnp.where(total(((way == w) & (dist > hop)).astype(f32)) > count * GROUP, 0.0, fits)
        start = 0
        for end, least, reach in phases:
            fits = jnp.where(total((dist < least).astype(f32)) > start * GROUP, 0.0, fits)
            fits = jnp.where(total((dist <= reach).astype(f32)) < end * GROUP, 0.0, fits)
            start = end
        return fits

    fits = [fitting(plan) for plan in PLANS[:-1]]
    choice = jnp.full((1, 1), float(len(PLANS) - 1), f32)
    for i in reversed(range(len(PLANS) - 1)):
        choice = jnp.where(fits[i] > 0, float(i), choice)

    chunk = jnp.floor(slot / GROUP)
    within = slot - chunk * GROUP
    spot = []
    for hops, _ in PLANS:
        at = jnp.zeros((1, blocks), f32)
        for hop in range(HALF):
            other = jnp.where(way == 2.0, float(store_size(hops, store_of(hop))), 0.0)
            at = jnp.where(dist == hop + 1, other + float(store_base(hops, hop)), at)
        spot.append(at + chunk)
    spot = functools.reduce(lambda rest, i: jnp.where(choice == i, spot[i], rest), range(len(PLANS) - 1), spot[-1])
    spot = jnp.where(way == 0, 0.0, spot)
    within = jnp.where(way == 0, 0.0, within)
    slot_c, way_c, source_c, place_c = column(slot), column(way), column(source), column(place)
    here = slot_c == lane2_f
    send = [down(jnp.where(here & (way_c == w), source_c, 0.0)) for w in (1.0, 2.0)]
    there = place_c == lane2_f

    def ordered(v):
        return down(jnp.where(there, column(v), 0.0))

    at = ordered(spot)
    inside = ordered(within)
    kind = ordered(dist)
    turn = 8.0 * (lane_f - GROUP * jnp.floor(lane_f / GROUP) - inside) + jnp.where(kind == 0, 4.0, 0.0)
    turn = jnp.where(turn < 0, turn + LANES, turn)
    rows = [
        send[0],
        send[1],
        at * PACKET + inside,
        at * PACKET + GROUP,
        turn,
        down(jnp.where(there, source_c, 0.0)),
        kind,
        down(jnp.where(there, sub2.astype(f32), 0.0)),
        place,
        spread(choice)[:1],
    ]
    rows += [jnp.zeros((1, blocks), f32)] * (16 - len(rows))
    tab_ref[...] = jnp.concatenate(rows, axis=0).astype(jnp.int32)


def exchange_kernel(plan, tab, ratios, pot, out, p1, p2, tiles, sent, got_a, got_b, got_c, got_d, v1, v2, near, c1s, turned,
                    local_sem, send_sem, recv_sem, edge_send, edge_recv):
    hops, phases = plan
    base, number = chunk_base(hops)
    stores = (got_a, got_b, got_c, got_d)
    size = lax.axis_size("row")
    stride = size // RB
    me = lax.axis_index("row")
    blocks = tiles.shape[0]
    rows = tiles.shape[1]
    tall = rows + 2 * EDGE
    first = hops[0]

    load2 = pltpu.make_async_copy(pot.at[1], p2, local_sem.at[0])
    load1 = pltpu.make_async_copy(pot.at[0], p1, local_sem.at[1])
    load2.start()
    load1.start()
    barrier = pltpu.get_barrier_semaphore()
    for by in (stride, size - stride, 1, size - 1):
        pl.semaphore_signal(barrier, inc=1, device_id={"row": lax.rem(me + by, size)}, device_id_type=MESH)

    lane = iota((rows, LANES), 1)
    lane_group = lane // 8

    def split(source, put):
        def body(i, carry):
            for j in range(GROUP):
                b = i * GROUP + j
                put(b, source[:, pl.ds(pl.multiple_of(b * LANES, LANES), LANES)])
            return carry

        lax.fori_loop(0, blocks // GROUP, body, 0)

    def put_tile(b, value):
        tiles[b] = value

    def put_v1(b, value):
        v1[b, EDGE : EDGE + rows, :] = value

    def sides(s):
        before = tiles[(s + (blocks - 1)) & (blocks - 1)]
        after = tiles[(s + 1) & (blocks - 1)]
        return jnp.where(lane >= LANES // 2, before, after)

    def pack(i):
        way = lax.rem(i, 2)
        chunk = i // 2
        halo = jnp.zeros((rows, LANES), jnp.float32)
        for j in range(GROUP):
            s = tab[way, chunk * GROUP + j]
            sent[i * PACKET + j] = tiles[s]
            halo = jnp.where(lane_group == j, pltpu.roll(sides(s), (8 * j + 4) % LANES, 1), halo)
        sent[i * PACKET + GROUP] = halo

    def first_copy(i):
        way = lax.rem(i, 2)
        to = way * number + i // 2
        land = way * store_size(hops, 0) + i // 2
        return pltpu.make_async_remote_copy(
            src_ref=sent.at[pl.ds(i * PACKET, PACKET)],
            dst_ref=got_a.at[pl.ds(land * PACKET, PACKET)],
            send_sem=send_sem.at[to],
            recv_sem=recv_sem.at[to],
            device_id={"row": lax.rem(me + jnp.where(way == 0, size - stride, stride), size)},
            device_id_type=MESH,
        )

    def piece(way, hop, c):
        where = store_of(hop)
        at = way * store_size(hops, where) + store_base(hops, hop) + c
        return stores[where].at[pl.ds(at * PACKET, PACKET)]

    def relay(way, hop, c):
        to = way * number + base[hop] + c
        return pltpu.make_async_remote_copy(
            src_ref=piece(way, hop - 1, c),
            dst_ref=piece(way, hop, c),
            send_sem=send_sem.at[to],
            recv_sem=recv_sem.at[to],
            device_id={"row": lax.rem(me + (size - stride if way == 0 else stride), size)},
            device_id_type=MESH,
        )

    def arrival(way, hop, c):
        to = way * number + base[hop] + c
        here = piece(way, hop, c)
        return pltpu.make_async_remote_copy(
            src_ref=here, dst_ref=here, send_sem=send_sem.at[to], recv_sem=recv_sem.at[to],
            device_id={"row": lax.rem(me + stride, size)}, device_id_type=MESH,
        )

    def edges(ref, begin, end, at):
        span = pl.ds(begin, end - begin)
        pair = []
        for k, (src, dst, by) in enumerate(((rows, 0, 1), (EDGE, EDGE + rows, size - 1))):
            pair.append(
                pltpu.make_async_remote_copy(
                    src_ref=ref.at[span, src : src + EDGE, :],
                    dst_ref=ref.at[span, dst : dst + EDGE, :],
                    send_sem=edge_send.at[2 * at + k],
                    recv_sem=edge_recv.at[2 * at + k],
                    device_id={"row": lax.rem(me + by, size)},
                    device_id_type=MESH,
                )
            )
        return pair

    load2.wait()
    split(p2, put_tile)
    pack(0)
    pl.semaphore_wait(barrier, 4)

    def step(i, carry):
        pack(i)
        first_copy(i - 1).start()
        return carry

    lax.fori_loop(1, 2 * first, step, 0)
    first_copy(2 * first - 1).start()

    load1.wait()
    split(p1, put_v1)
    edges1 = edges(v1, 0, blocks, 0)
    for copy in edges1:
        copy.start()

    near_far, beta_one, beta_two = ratios[0], ratios[1], ratios[2]
    one = 1.0 / 12.0
    two = 1.0 / 144.0

    def second(x, s1, s2, s3, s4):
        return 16.0 * (s1 - s3) + 64.0 * s2 + s4 - 130.0 * x

    sub = iota((8, LANES), 0)
    lane8 = iota((8, LANES), 1)
    eight = rows // 2

    def thirds(ref, f):
        even = ref[f, pl.ds(EDGE, eight, stride=2), :]
        odd = ref[f, pl.ds(EDGE + 1, eight, stride=2), :]
        return even, odd, jnp.where(sub < EDGE, ref[f, 0:8, :], ref[f, tall - 8 : tall, :])

    def derive(ref, f, t, j):
        x = thirds(ref, f)

        def ahead(p, k):
            return pltpu.roll(jnp.where(lane8 < k, t[p], x[p]), LANES - k, 1)

        def behind(p, k):
            return pltpu.roll(jnp.where(lane8 >= LANES - k, t[p], x[p]), k, 1)

        slope_c, curve_cc = [], []
        for p in range(3):
            a1, b1, a2, b2 = ahead(p, 1), behind(p, 1), ahead(p, 2), behind(p, 2)
            slope_c.append(8.0 * (a1 - b1) - (a2 - b2))
            if p < 2:
                curve_cc.append(second(x[p], a1 + b1, a2 + b2, ahead(p, 3) + behind(p, 3), ahead(p, 4) + behind(p, 4)))
        for p in range(2):
            c1s[j, pl.ds(EDGE + p, eight, stride=2), :] = slope_c[p]
        c1s[j, 0:EDGE, :] = slope_c[2][:EDGE]
        c1s[j, tall - EDGE : tall, :] = slope_c[2][EDGE:]
        c = {EDGE: slope_c[0], EDGE + 1: slope_c[1]}
        r = {EDGE: x[0], EDGE + 1: x[1]}
        for at in (2, 3, 6, 7):
            c[at] = c1s[j, pl.ds(at, eight, stride=2), :]
        for at in (0, 1, 2, 3, 6, 7, 8, 9):
            r[at] = ref[f, pl.ds(at, eight, stride=2), :]
        slope_r, curve_rr, curve_rc = [], [], []
        for p in range(2):
            m = EDGE + p
            slope_r.append(8.0 * (r[m + 1] - r[m - 1]) - (r[m + 2] - r[m - 2]))
            curve_rr.append(second(r[m], *[r[m + k] + r[m - k] for k in range(1, 5)]))
            curve_rc.append(8.0 * (c[m + 1] - c[m - 1]) - (c[m + 2] - c[m - 2]))
        return slope_r, slope_c, curve_rr, curve_rc, curve_cc

    def near_group(g):
        for j in range(GROUP):
            b = g * GROUP + j
            before = thirds(v1, b - 1 if j > 0 else lax.rem(b + (blocks - 1), blocks))
            after = thirds(v1, b + 1 if j < GROUP - 1 else lax.rem(b + 1, blocks))
            t = [jnp.where(lane8 >= LANES // 2, before[p], after[p]) for p in range(3)]
            slope_r, slope_c, curve_rr, curve_rc, curve_cc = derive(v1, b, t, j)
            for p in range(2):
                values = (
                    two * (curve_rr[p] + curve_cc[p]),
                    two * (curve_cc[p] - curve_rr[p]),
                    (2.0 * two) * curve_rc[p],
                    (one * beta_one) * slope_r[p],
                    (one * beta_one) * slope_c[p],
                )
                for k, value in enumerate(values):
                    near[b, k * rows + p * eight : k * rows + (p + 1) * eight, :] = value

    def near_groups(begin, end):
        def body(g, carry):
            near_group(g)
            return carry

        lax.fori_loop(begin, end, body, 0)

    def gather(begin, end, kinds):
        def body(g, carry):
            halo = jnp.zeros((rows, LANES), jnp.float32)
            for j in range(GROUP):
                f = g * GROUP + j
                kind = jnp.full((rows, LANES), tab[6, f], jnp.int32)
                value = cols = None
                for k in kinds:
                    if k == 0:
                        s = tab[5, f]
                        v, c = tiles[s], sides(s)
                    else:
                        ref = stores[k - 1]
                        at_v, at_c = tab[2, f], tab[3, f]
                        if any(k2 > 0 and stores[k2 - 1].shape[0] > ref.shape[0] for k2 in kinds):
                            at_v, at_c = jnp.minimum(at_v, ref.shape[0] - 1), jnp.minimum(at_c, ref.shape[0] - 1)
                        v, c = ref[at_v], ref[at_c]
                    value = v if value is None else jnp.where(kind == k, v, value)
                    cols = c if cols is None else jnp.where(kind == k, c, cols)
                halo = jnp.where(lane_group == j, pltpu.roll(cols, tab[4, f], 1), halo)
                v2[g * PACKET + j, EDGE : EDGE + rows, :] = value
            v2[g * PACKET + GROUP, EDGE : EDGE + rows, :] = halo
            return carry

        lax.fori_loop(begin, end, body, 0)

    scale = 0.5 * two * beta_two
    half_far = 0.5 * near_far
    half_one = 0.5 * beta_one
    slope_scale = one * beta_two

    def combine(begin, end):
        def body(g, carry):
            halo = thirds(v2, g * PACKET + GROUP)
            for j in range(GROUP):
                for p in range(3):
                    turned[j, 8 * p : 8 * p + 8, :] = pltpu.roll(halo[p], (LANES - 8 * j - 4) % LANES, 1)
            for j in range(GROUP):
                f = g * GROUP + j
                t = [turned[j, 8 * p : 8 * p + 8, :] for p in range(3)]
                far_r, far_c, far_rr, far_rc, far_cc = derive(v2, g * PACKET + j, t, j)
                n = near[tab[7, f]]
                for p in range(2):
                    n_sum, n_diff, n_rc2, n_r, n_c = (
                        n[k * rows + p * eight : k * rows + (p + 1) * eight] for k in range(5)
                    )
                    s = scale * (far_rr[p] + far_cc[p])
                    d = scale * (far_cc[p] - far_rr[p])
                    r = scale * far_rc[p]
                    d_half = half_far * d
                    r_far = near_far * r
                    rest = half_one - half_far * s
                    results = (
                        s + n_sum * rest - d_half * n_diff - r_far * n_rc2,
                        d + n_diff * rest - d_half * n_sum,
                        (r + r) + n_rc2 * rest - r_far * n_sum,
                        r_far * n_diff - n_rc2 * d_half,
                        n_r + slope_scale * far_r[p],
                        n_c + slope_scale * far_c[p],
                    )
                    for k, value in enumerate(results):
                        out[f, pl.ds(k * rows + p, eight, stride=2), :] = value
            return carry

        lax.fori_loop(begin, end, body, 0)

    def forward(hop, c):
        for way in range(2):
            arrival(way, hop - 1, c).wait_recv()
            relay(way, hop, c).start()

    def land(hop):
        for c in range(hops[hop + 1] if hop + 1 < HALF else 0, hops[hop]):
            for way in range(2):
                arrival(way, hop, c).wait_recv()

    groups = blocks // GROUP
    bounds = [0] + [end for end, _, _ in phases]
    moved = [edges(v2, bounds[p] * PACKET, bounds[p + 1] * PACKET, 1 + p) for p in range(len(phases))]
    landed = set()

    def begin_phase(p):
        _, least, reach = phases[p]
        for hop in range(reach):
            if hop not in landed:
                land(hop)
                landed.add(hop)
        gather(bounds[p], bounds[p + 1], range(least, reach + 1))
        for copy in moved[p]:
            copy.start()

    def end_phase(p):
        for copy in moved[p]:
            copy.wait_recv()
        combine(bounds[p], bounds[p + 1])

    if len(phases) < 3:
        for hop in range(1, HALF):
            for c in range(hops[hop]):
                forward(hop, c)
        for copy in edges1:
            copy.wait_recv()
        near_groups(0, groups)
        for p in range(len(phases)):
            begin_phase(p)
            end_phase(p)
    else:
        early = [(hop, c) for hop in (1, 2) for c in range(hops[hop])]
        share = -(-groups // (len(early) - 1))
        done = began = 0
        for i, (hop, c) in enumerate(early):
            forward(hop, c)
            if i == 0:
                for copy in edges1:
                    copy.wait_recv()
            upto = min(groups, done + share)
            if upto > done:
                near_groups(done, upto)
            done = upto
            if phases[0][2] == 1 and i == hops[1] - 1:
                begin_phase(0)
                began = 1
        if began:
            end_phase(0)
        begin_phase(began)
        for c in range(hops[3]):
            forward(3, c)
        end_phase(began)
        for p in range(began + 1, len(phases)):
            begin_phase(p)
            if p > began + 1:
                end_phase(p - 1)
        end_phase(len(phases) - 1)

    for copy in edges1:
        copy.wait_send()
    for pair in moved:
        for copy in pair:
            copy.wait_send()
    for way in range(2):
        for hop in range(HALF):
            for c in range(hops[hop]):
                arrival(way, hop, c).wait_send()


def exchange(index, tab, ratios, potentials):
    plan = PLANS[index]
    hops, phases = plan
    rows, columns = potentials.shape[1:]
    blocks = columns // LANES
    _, number = chunk_base(hops)
    packets = blocks // GROUP * PACKET
    tall = rows + 2 * EDGE
    f32 = jnp.float32
    smem = pl.BlockSpec(memory_space=pltpu.SMEM)
    return pl.pallas_call(
        functools.partial(exchange_kernel, plan),
        out_shape=jax.ShapeDtypeStruct((blocks, 6 * rows, LANES), f32),
        in_specs=[smem, smem, pl.BlockSpec(memory_space=pl.ANY)],
        out_specs=pl.BlockSpec(memory_space=pltpu.VMEM),
        scratch_shapes=[
            pltpu.VMEM((rows, columns), f32),
            pltpu.VMEM((rows, columns), f32),
            pltpu.VMEM((blocks, rows, LANES), f32),
            pltpu.VMEM((2 * hops[0] * PACKET, rows, LANES), f32),
            *[pltpu.VMEM((2 * store_size(hops, i) * PACKET, rows, LANES), f32) for i in range(len(STORES))],
            pltpu.VMEM((blocks, tall, LANES), f32),
            pltpu.VMEM((packets, tall, LANES), f32),
            pltpu.VMEM((blocks, 5 * rows, LANES), f32),
            pltpu.VMEM((GROUP, tall, LANES), f32),
            pltpu.VMEM((GROUP, tall, LANES), f32),
            pltpu.SemaphoreType.DMA((2,)),
            pltpu.SemaphoreType.DMA((2 * number,)),
            pltpu.SemaphoreType.DMA((2 * number,)),
            pltpu.SemaphoreType.DMA((2 + 2 * len(phases),)),
            pltpu.SemaphoreType.DMA((2 + 2 * len(phases),)),
        ],
        compiler_params=pltpu.CompilerParams(
            collective_id=index, has_side_effects=True, vmem_limit_bytes=30 * 2**20
        ),
        name=f"exchange{index}",
    )(tab, ratios, potentials)


def arrange_kernel(tab, fields, conv, shear, rot, disp):
    g = pl.program_id(0)
    rows, wide = conv.shape
    for j in range(wide // LANES):
        value = fields[tab[8, g * (wide // LANES) + j]]
        part = [value[k * rows : (k + 1) * rows] for k in range(6)]
        spot = slice(j * LANES, (j + 1) * LANES)
        conv[:, spot] = part[0]
        shear[0, :, spot] = part[1]
        shear[1, :, spot] = part[2]
        rot[:, spot] = part[3]
        disp[0, :, spot] = part[4]
        disp[1, :, spot] = part[5]


def arrange(tab, fields, rows):
    columns = fields.shape[0] * LANES
    wide = columns // 2
    f32 = jnp.float32
    flat = jax.ShapeDtypeStruct((rows, columns), f32)
    pair = jax.ShapeDtypeStruct((2, rows, columns), f32)
    flat_spec = pl.BlockSpec((rows, wide), lambda g: (0, g))
    pair_spec = pl.BlockSpec((2, rows, wide), lambda g: (0, 0, g))
    return pl.pallas_call(
        arrange_kernel,
        grid=(columns // wide,),
        out_shape=(flat, pair, flat, pair),
        in_specs=[pl.BlockSpec(memory_space=pltpu.SMEM), pl.BlockSpec(memory_space=pltpu.VMEM)],
        out_specs=(flat_spec, pair_spec, flat_spec, pair_spec),
        compiler_params=pltpu.CompilerParams(vmem_limit_bytes=16 * 2**20),
        name="arrange",
    )(tab, fields)


def per_device(potentials, ratios, row_offset, col_offset):
    blocks = row_offset.shape[0]
    vmem = pl.BlockSpec(memory_space=pltpu.VMEM)
    tab = pl.pallas_call(
        table_kernel,
        out_shape=jax.ShapeDtypeStruct((16, blocks), jnp.int32),
        in_specs=[vmem, vmem],
        out_specs=vmem,
        name="table",
    )(row_offset.reshape(1, blocks), col_offset.reshape(1, blocks))
    def run(index, tab, ratios, potentials):
        return arrange(tab, exchange(index, tab, ratios, potentials), potentials.shape[1])

    return lax.switch(
        tab[9, 0], [functools.partial(run, i) for i in range(len(PLANS))], tab, ratios, potentials
    )


def solution(mesh):
    return jax.shard_map(
        per_device,
        mesh=mesh,
        in_specs=(P("cosmo", "row", None), P("cosmo"), P("cosmo"), P("cosmo")),
        out_specs=(
            P(("cosmo", "row"), None),
            P(None, ("cosmo", "row"), None),
            P(("cosmo", "row"), None),
            P(None, ("cosmo", "row"), None),
        ),
        check_vma=False,
    )
```
